8 devices in a mesh: slab: 2 (over z, y), col: 2 (over x), row: 2 (over core).
Axes of the slice: x: 2, y: 2, z: 1, core: 2. Of those that a mesh axis runs over, the one named last changes fastest.
Arguments:
- tensor: bfloat16 [32, 256, 256, 256], P(None, 'row', 'col', 'slab')
- factor_one: float32 [256, 16], replicated
- factor_two: float32 [256, 16], replicated
- factor_three: float32 [256, 16], replicated
Outputs:
- output 1: float32 [32, 16, 16, 16], P(None, 'row', 'col', 'slab')
- output 2: float32 [32], replicated
All inputs are finite; a program needn't handle non-finite values.
Results may differ from the reference program's by a relative error of at most 0.001.
Values are sent between devices in bfloat16 or wider.
A program may use at most 1 GiB of HBM per device.

```python
import jax
import jax.numpy as jnp
from jax import lax
import math

SNAPS = 32
I1 = 256
I2 = 256
I3 = 256
R1 = 16
R2 = 16
R3 = 16


def orth_columns(mat):
    return jnp.linalg.qr(mat)[0]


def setup_inputs(seed: int = 0) -> dict:
    key_list = jax.random.split(jax.random.key(seed), 8)
    sig_one = orth_columns(jax.random.normal(key_list[0], (I1, R1), jnp.float32))
    sig_two = orth_columns(jax.random.normal(key_list[1], (I2, R2), jnp.float32))
    sig_three = orth_columns(jax.random.normal(key_list[2], (I3, R3), jnp.float32))
    factor_one = orth_columns(0.9 * sig_one + 0.44 / math.sqrt(I1) * jax.random.normal(key_list[3], (I1, R1), jnp.float32))
    factor_two = orth_columns(0.9 * sig_two + 0.44 / math.sqrt(I2) * jax.random.normal(key_list[4], (I2, R2), jnp.float32))
    factor_three = orth_columns(0.9 * sig_three + 0.44 / math.sqrt(I3) * jax.random.normal(key_list[5], (I3, R3), jnp.float32))
    noise_scale = math.sqrt(0.5 * R1 * R2 * R3 / (I1 * I2 * I3))

    def one_snap(snap_index):
        core_sig = jax.random.normal(jax.random.fold_in(key_list[6], snap_index), (R1, R2, R3), jnp.float32)
        stage_a = jnp.einsum('abc,ia->ibc', core_sig, sig_one)
        stage_b = jnp.einsum('ibc,jb->ijc', stage_a, sig_two)
        signal = jnp.dot(stage_b.reshape(I1 * I2, R3), sig_three.T).reshape(I1, I2, I3)
        noise_part = jax.random.normal(jax.random.fold_in(key_list[7], snap_index), (I1, I2, I3), jnp.float32)
        return (signal + noise_scale * noise_part).astype(jnp.bfloat16)

    tensor = lax.map(one_snap, jnp.arange(SNAPS))
    return {'tensor': tensor, 'factor_one': factor_one, 'factor_two': factor_two, 'factor_three': factor_three}


def compress_snapshot(x_snap, bf_one, bf_two, bf_three):
    stage_a = jnp.dot(x_snap.reshape(I1 * I2, I3), bf_three, preferred_element_type=jnp.float32)
    stage_a = stage_a.astype(jnp.bfloat16).reshape(I1, I2, R3)
    stage_b = jnp.einsum('ijc,jb->ibc', stage_a.astype(jnp.float32), bf_two.astype(jnp.float32)).astype(jnp.bfloat16)
    core_snap = jnp.einsum('ibc,ia->abc', stage_b.astype(jnp.float32), bf_one.astype(jnp.float32))
    x_energy = jnp.sum(jnp.square(x_snap.astype(jnp.float32)))
    g_energy = jnp.sum(jnp.square(core_snap))
    return core_snap, (x_energy - g_energy) / x_energy


def reference(tensor, factor_one, factor_two, factor_three):
    bf_one = factor_one.astype(jnp.bfloat16)
    bf_two = factor_two.astype(jnp.bfloat16)
    bf_three = factor_three.astype(jnp.bfloat16)
    core_tensor, rel_error = lax.map(lambda x_snap: compress_snapshot(x_snap, bf_one, bf_two, bf_three), tensor)
    return core_tensor, rel_error
```

```python
import functools

import jax
import jax.numpy as jnp
from jax import lax
from jax.experimental import pallas as pl
from jax.experimental.pallas import tpu as pltpu
from jax.sharding import PartitionSpec as P

MESH = pl.DeviceIdType.MESH
F32, BF16 = jnp.float32, jnp.bfloat16
NT = (((1,), (1,)), ((), ()))

LAG = 4
RING = 2 * LAG
XBUF = 4
BRING = 4
SUB = 8


def other(axis):
    return {axis: 1 - lax.axis_index(axis)}


def offset_peer(dd):
    peer = {}
    for bit, axis in ((4, 'slab'), (2, 'col'), (1, 'row')):
        here = lax.axis_index(axis)
        peer[axis] = 1 - here if dd & bit else here
    return peer


def tree(parts):
    while len(parts) > 1:
        parts = [parts[k] + parts[k + 1] for k in range(0, len(parts), 2)]
    return parts[0]


def kernel(snaps, rows, x_hbm, f1_hbm, f2_hbm, f3_hbm, g_out, e_out,
           xbuf, f1, f2, f3, u3w, u2w, w1, own, ysend, yrecv, bown, xsend, xrecv,
           gpart, grecv, ex, exg, eg, x_sem, f_sem, ys_sem, yr_sem, xs_sem, xr_sem, g_sem, ex_ssem, ex_rsem, eg_ssem, eg_rsem):
    nq = 128 // rows
    nc = snaps * nq
    width = rows * 8
    slab, col, row = (lax.axis_index(a) for a in ('slab', 'col', 'row'))

    def x_copy(c):
        slot = lax.rem(c, XBUF)
        return pltpu.make_async_copy(x_hbm.at[c], xbuf.at[slot], x_sem.at[slot])

    f_copies = [pltpu.make_async_copy(src, dst, f_sem.at[k]) for k, (src, dst) in enumerate(((f3_hbm, f3), (f2_hbm, f2), (f1_hbm, f1)))]
    f_copies[0].start()
    for c in range(XBUF):
        x_copy(c).start()
    f_copies[1].start()
    f_copies[2].start()

    barrier = pltpu.get_barrier_semaphore()
    for dd in range(1, 8):
        pl.semaphore_signal(barrier, inc=1, device_id=offset_peer(dd), device_id_type=MESH)

    def swapped(block, flip):
        return jnp.where(flip == 0, block, jnp.concatenate([block[8:], block[:8]], axis=0)).astype(BF16)

    f_copies[0].wait()
    u3w[...] = swapped(f3[:, pl.ds(pl.multiple_of(slab * 128, 128), 128)], slab)
    ex[...] = jnp.zeros_like(ex)
    pl.semaphore_wait(barrier, 7)

    def y_copy(c):
        slot = lax.rem(c, RING)
        return pltpu.make_async_remote_copy(ysend.at[slot], yrecv.at[slot], ys_sem.at[slot], yr_sem.at[slot], device_id=other('slab'), device_id_type=MESH)

    def b_copy(c):
        slot = lax.rem(c, BRING)
        return pltpu.make_async_remote_copy(xsend.at[slot], xrecv.at[slot], xs_sem.at[slot], xr_sem.at[slot], device_id=other('col'), device_id_type=MESH)

    def ex_copy(dd):
        return pltpu.make_async_remote_copy(exg.at[0], exg.at[dd], ex_ssem.at[dd], ex_rsem.at[dd], device_id=offset_peer(dd), device_id_type=MESH)

    def eg_copy(dd):
        return pltpu.make_async_remote_copy(eg.at[0], eg.at[dd // 2], eg_ssem.at[dd // 2], eg_rsem.at[dd // 2], device_id=offset_peer(dd), device_id_type=MESH)

    g_copy = pltpu.make_async_remote_copy(gpart, grecv, g_sem.at[0], g_sem.at[1], device_id=other('row'), device_id_type=MESH)

    def mode_three(c):
        slot, xs = lax.rem(c, RING), lax.rem(c, XBUF)
        x_copy(c).wait()

        @pl.when(c >= RING)
        def _():
            y_copy(c).wait_send()

        def block(k, acc):
            x = xbuf[xs, pl.ds(pl.multiple_of(k * SUB * 128, SUB * 128), SUB * 128), :]
            part = lax.dot_general(u3w[...], x, NT, preferred_element_type=F32)
            for i in range(SUB):
                own[slot, k * SUB + i] = part[:8, i * 128:(i + 1) * 128]
                ysend[slot, k * SUB + i] = part[8:, i * 128:(i + 1) * 128]
            xf = x.astype(F32).reshape(-1, 4, 8, 128)
            return acc + jnp.sum(xf * xf, axis=0)

        acc = lax.fori_loop(0, rows // SUB, block, jnp.zeros((4, 8, 128), F32))
        t = lax.div(c, nq)
        ex[t] += jnp.sum(acc, axis=0)

        @pl.when(c + XBUF < nc)
        def _():
            x_copy(c + XBUF).start()

    def mode_two(c):
        slot, bslot = lax.rem(c, RING), lax.rem(c, BRING)
        y_copy(c).wait_recv()

        @pl.when(c >= BRING)
        def _():
            b_copy(c).wait_send()

        a = (own[slot] + yrecv[slot]).reshape(width, 128).astype(BF16)
        part = lax.dot_general(u2w[...], a, NT, preferred_element_type=F32)
        bown[bslot] = part[:8]
        xsend[bslot] = part[8:]

    def mode_one(c):
        bslot = lax.rem(c, BRING)
        b_copy(c).wait_recv()
        b = (bown[bslot] + xrecv[bslot]).astype(BF16)
        q, t = lax.rem(c, nq), lax.div(c, nq)
        g = jnp.dot(b, w1[q], preferred_element_type=F32)

        @pl.when(q == 0)
        def _():
            gpart[t] = g

        @pl.when(q > 0)
        def _():
            gpart[t] += g

    def late_setup():
        f_copies[1].wait()
        f_copies[2].wait()
        u2w[...] = swapped(f2[:, pl.ds(pl.multiple_of(col * 128, 128), 128)], col)
        u1 = f1[:, pl.ds(pl.multiple_of(row * 128, 128), 128)].astype(BF16)
        spread = (lax.broadcasted_iota(jnp.int32, (16, 128), 1) // 8 == lax.broadcasted_iota(jnp.int32, (16, 128), 0)).astype(BF16)
        r = lax.broadcasted_iota(jnp.int32, (width, 128), 0)
        l = lax.broadcasted_iota(jnp.int32, (width, 128), 1)
        for q in range(nq):
            pick = (l == q * rows + r // 8).astype(BF16)
            rowed = lax.dot_general(pick, u1, NT, preferred_element_type=F32).astype(BF16)
            wide = jnp.dot(rowed, spread, preferred_element_type=F32)
            w1[q] = jnp.where(r % 8 == l % 8, wide, 0.0).astype(BF16)

    def step(s, carry):
        @pl.when((s >= 1) & (s <= nc))
        def _():
            y_copy(s - 1).start()

        @pl.when(s >= LAG + 1)
        def _():
            b_copy(s - LAG - 1).start()

        @pl.when(s < nc)
        def _():
            mode_three(s)

        @pl.when(s == 2)
        def _():
            late_setup()

        @pl.when(s == nc)
        def _():
            exg[0] = jnp.broadcast_to(jnp.sum(jnp.sum(ex[...], axis=1), axis=1, keepdims=True), (snaps, 128))

        @pl.when(s == nc + 1)
        def _():
            for dd in range(1, 8):
                ex_copy(dd).start()

        @pl.when((s >= LAG) & (s < nc + LAG))
        def _():
            mode_two(s - LAG)

        @pl.when(s >= LAG + 1)
        def _():
            mode_one(s - LAG - 1)

        return carry

    lax.fori_loop(0, nc + LAG + 1, step, 0)

    g_copy.start()
    for c in range(nc - RING, nc):
        y_copy(c).wait_send()
    for c in range(nc - BRING, nc):
        b_copy(c).wait_send()
    for dd in range(1, 8):
        ex_copy(dd).wait()
    x_energy = tree([exg[dd] for dd in range(8)])
    g_copy.wait()

    g = gpart[...] + grecv[...]
    eg[0] = jnp.broadcast_to(jnp.sum(jnp.sum(g * g, axis=1), axis=1, keepdims=True), (snaps, 128))
    for dd in (2, 4, 6):
        eg_copy(dd).start()
    for b in range(8):
        turned = g[:, b, :].T
        g_out[:, b] = jnp.where(row == 0, turned[:64], turned[64:]).reshape(8, 8, snaps)
    for dd in (2, 4, 6):
        eg_copy(dd).wait()
    g_energy = tree([eg[k] for k in range(4)])
    rel = (x_energy - g_energy) / x_energy
    diag = lax.broadcasted_iota(jnp.int32, (snaps, 128), 0) == lax.broadcasted_iota(jnp.int32, (snaps, 128), 1)
    e_out[...] = jnp.sum(jnp.where(diag, rel, 0.0), axis=0, keepdims=True)[:, :snaps]


def solution(mesh):
    rows = 32

    def local_part(x_block, f_one, f_two, f_three):
        snaps = x_block.shape[0]
        nq = 128 // rows
        nc = snaps * nq
        dma = pltpu.SemaphoreType.DMA
        hbm = pl.BlockSpec(memory_space=pl.ANY)
        vmem = pl.BlockSpec(memory_space=pltpu.VMEM)
        g, e = pl.pallas_call(
            functools.partial(kernel, snaps, rows),
            out_shape=(jax.ShapeDtypeStruct((8, 8, 8, snaps), F32), jax.ShapeDtypeStruct((1, snaps), F32)),
            in_specs=[hbm] * 4,
            out_specs=(vmem, vmem),
            scratch_shapes=[
                pltpu.VMEM((XBUF, rows * 128, 128), BF16),
                pltpu.VMEM((16, 256), F32), pltpu.VMEM((16, 256), F32), pltpu.VMEM((16, 256), F32),
                pltpu.VMEM((16, 128), BF16), pltpu.VMEM((16, 128), BF16),
                pltpu.VMEM((nq, rows * 8, 128), BF16),
                pltpu.VMEM((RING, rows, 8, 128), F32), pltpu.VMEM((RING, rows, 8, 128), F32), pltpu.VMEM((RING, rows, 8, 128), F32),
                pltpu.VMEM((BRING, 8, rows * 8), F32), pltpu.VMEM((BRING, 8, rows * 8), F32), pltpu.VMEM((BRING, 8, rows * 8), F32),
                pltpu.VMEM((snaps, 8, 128), F32), pltpu.VMEM((snaps, 8, 128), F32),
                pltpu.VMEM((snaps, 8, 128), F32), pltpu.VMEM((8, snaps, 128), F32), pltpu.VMEM((4, snaps, 128), F32),
                dma((XBUF,)), dma((3,)), dma((RING,)), dma((RING,)), dma((BRING,)), dma((BRING,)), dma((2,)), dma((8,)), dma((8,)), dma((4,)), dma((4,)),
            ],
            compiler_params=pltpu.CompilerParams(collective_id=0, has_side_effects=True),
        )(x_block.reshape(nc, rows * 128, 128), f_one.T, f_two.T, f_three.T)
        return g.transpose(3, 0, 1, 2), e.reshape(snaps)

    return jax.shard_map(local_part, mesh=mesh, in_specs=(P(None, 'row', 'col', 'slab'), P(None, None), P(None, None), P(None, None)), out_specs=(P(None, 'row', 'col', 'slab'), P()), check_vma=False)
```

```python
import functools

import jax
import jax.numpy as jnp
from jax import lax
from jax.experimental import pallas as pl
from jax.experimental.pallas import tpu as pltpu
from jax.sharding import PartitionSpec as P

MESH = pl.DeviceIdType.MESH
F32, BF16 = jnp.float32, jnp.bfloat16
NT = (((1,), (1,)), ((), ()))

LAG = 4
RING = 2 * LAG
XBUF = 4
BRING = 4
SUB = 8


def other(axis):
    return {axis: 1 - lax.axis_index(axis)}


def offset_peer(dd):
    peer = {}
    for bit, axis in ((4, 'slab'), (2, 'col'), (1, 'row')):
        here = lax.axis_index(axis)
        peer[axis] = 1 - here if dd & bit else here
    return peer


def tree(parts):
    while len(parts) > 1:
        parts = [parts[k] + parts[k + 1] for k in range(0, len(parts), 2)]
    return parts[0]


def kernel(snaps, rows, x_hbm, f1_hbm, f2_hbm, f3_hbm, g_out, e_out,
           xbuf, f1, f2, f3, u3w, u2w, w1, own, ysend, yrecv, bown, xsend, xrecv,
           gpart, grecv, ex, energy, glast, x_sem, f_sem, ys_sem, yr_sem, xs_sem, xr_sem, g_sem, en_ssem, en_rsem, gl_ssem, gl_rsem):
    nq = 128 // rows
    nc = snaps * nq
    width = rows * 8
    last = snaps - 1
    slab, col, row = (lax.axis_index(a) for a in ('slab', 'col', 'row'))

    def x_copy(c):
        slot = lax.rem(c, XBUF)
        return pltpu.make_async_copy(x_hbm.at[c], xbuf.at[slot], x_sem.at[slot])

    f_copies = [pltpu.make_async_copy(src, dst, f_sem.at[k]) for k, (src, dst) in enumerate(((f3_hbm, f3), (f2_hbm, f2), (f1_hbm, f1)))]
    f_copies[0].start()
    x_copy(0).start()

    barrier = pltpu.get_barrier_semaphore()
    for dd in (4, 2, 1):
        pl.semaphore_signal(barrier, inc=1, device_id=offset_peer(dd), device_id_type=MESH)

    def swapped(block, flip):
        return jnp.where(flip == 0, block, jnp.concatenate([block[8:], block[:8]], axis=0)).astype(BF16)

    f_copies[0].wait()
    u3w[...] = swapped(f3[:, pl.ds(pl.multiple_of(slab * 128, 128), 128)], slab)
    ex[...] = jnp.zeros_like(ex)

    def y_copy(c):
        slot = lax.rem(c, RING)
        return pltpu.make_async_remote_copy(ysend.at[slot], yrecv.at[slot], ys_sem.at[slot], yr_sem.at[slot], device_id=other('slab'), device_id_type=MESH)

    def b_copy(c):
        slot = lax.rem(c, BRING)
        return pltpu.make_async_remote_copy(xsend.at[slot], xrecv.at[slot], xs_sem.at[slot], xr_sem.at[slot], device_id=other('col'), device_id_type=MESH)

    def energy_copy(dd):
        return pltpu.make_async_remote_copy(energy.at[0], energy.at[dd], en_ssem.at[dd], en_rsem.at[dd], device_id=offset_peer(dd), device_id_type=MESH)

    def last_copy(dd):
        return pltpu.make_async_remote_copy(gpart.at[last], glast.at[dd], gl_ssem.at[dd], gl_rsem.at[dd], device_id=offset_peer(dd), device_id_type=MESH)

    early = pl.ds(0, last)
    g_copy = pltpu.make_async_remote_copy(gpart.at[early], grecv.at[early], g_sem.at[0], g_sem.at[1], device_id=other('row'), device_id_type=MESH)

    def mode_three(c):
        slot, xs = lax.rem(c, RING), lax.rem(c, XBUF)
        x_copy(c).wait()

        @pl.when(c >= RING)
        def _():
            y_copy(c).wait_send()

        def block(k, acc):
            x = xbuf[xs, pl.ds(pl.multiple_of(k * SUB * 128, SUB * 128), SUB * 128), :]
            part = lax.dot_general(u3w[...], x, NT, preferred_element_type=F32)
            for i in range(SUB):
                own[slot, k * SUB + i] = part[:8, i * 128:(i + 1) * 128]
                ysend[slot, k * SUB + i] = part[8:, i * 128:(i + 1) * 128]
            xf = x.astype(F32).reshape(-1, 4, 8, 128)
            return acc + jnp.sum(xf * xf, axis=0)

        acc = lax.fori_loop(0, rows // SUB, block, jnp.zeros((4, 8, 128), F32))
        t = lax.div(c, nq)
        ex[t] += jnp.sum(acc, axis=0)

        @pl.when(c + XBUF < nc)
        def _():
            x_copy(c + XBUF).start()

    def mode_two(c):
        slot, bslot = lax.rem(c, RING), lax.rem(c, BRING)
        y_copy(c).wait_recv()

        @pl.when(c >= BRING)
        def _():
            b_copy(c).wait_send()

        a = (own[slot] + yrecv[slot]).reshape(width, 128).astype(BF16)
        part = lax.dot_general(u2w[...], a, NT, preferred_element_type=F32)
        bown[bslot] = part[:8]
        xsend[bslot] = part[8:]
        b_copy(c).start()

    def mode_one(c):
        bslot = lax.rem(c, BRING)
        b_copy(c).wait_recv()
        b = (bown[bslot] + xrecv[bslot]).astype(BF16)
        q, t = lax.rem(c, nq), lax.div(c, nq)
        g = jnp.dot(b, w1[q], preferred_element_type=F32)

        @pl.when(q == 0)
        def _():
            gpart[t] = g

        @pl.when(q > 0)
        def _():
            gpart[t] += g

    def late_setup():
        f_copies[1].wait()
        f_copies[2].wait()
        u2w[...] = swapped(f2[:, pl.ds(pl.multiple_of(col * 128, 128), 128)], col)
        u1 = f1[:, pl.ds(pl.multiple_of(row * 128, 128), 128)].astype(BF16)
        spread = (lax.broadcasted_iota(jnp.int32, (16, 128), 1) // 8 == lax.broadcasted_iota(jnp.int32, (16, 128), 0)).astype(BF16)
        r = lax.broadcasted_iota(jnp.int32, (width, 128), 0)
        l = lax.broadcasted_iota(jnp.int32, (width, 128), 1)
        for q in range(nq):
            pick = (l == q * rows + r // 8).astype(BF16)
            rowed = lax.dot_general(pick, u1, NT, preferred_element_type=F32).astype(BF16)
            wide = jnp.dot(rowed, spread, preferred_element_type=F32)
            w1[q] = jnp.where(r % 8 == l % 8, wide, 0.0).astype(BF16)

    def as_row(column, count):
        i = lax.broadcasted_iota(jnp.int32, (count, 128), 0)
        return jnp.sum(jnp.where(i == lax.broadcasted_iota(jnp.int32, (count, 128), 1), column, 0.0), axis=0, keepdims=True)

    def row_sums(blocks):
        return as_row(jnp.sum(jnp.sum(blocks, axis=1), axis=1, keepdims=True), blocks.shape[0])

    def step(s, carry):
        @pl.when((s >= 2) & (s <= nc))
        def _():
            y_copy(s - 1).start()

        @pl.when(s < nc)
        def _():
            mode_three(s)

        @pl.when(s == 2)
        def _():
            late_setup()

        @pl.when(s == nc)
        def _():
            energy[0, :1] = row_sums(ex[...])

        @pl.when(s == nc + LAG - 3)
        def _():
            g_copy.start()

        @pl.when((s >= LAG) & (s < nc + LAG))
        def _():
            mode_two(s - LAG)

        @pl.when(s == nc + LAG - 2)
        def _():
            g_copy.wait()
            g = gpart[early] + grecv[early]
            grecv[early] = g
            energy[0, 1:] = row_sums(g * g)

        @pl.when(s == nc + LAG - 1)
        def _():
            for dd in range(1, 8):
                energy_copy(dd).start()

        @pl.when(s >= LAG + 1)
        def _():
            mode_one(s - LAG - 1)

        return carry

    mode_three(0)
    pl.semaphore_wait(barrier, 3)
    y_copy(0).start()
    for c in range(1, XBUF):
        x_copy(c).start()
    f_copies[1].start()
    f_copies[2].start()
    lax.fori_loop(1, nc + LAG + 1, step, 0)

    for dd in (6, 7, 4, 5, 2, 3, 1):
        last_copy(dd).start()
    for c in range(nc - RING, nc):
        y_copy(c).wait_send()
    for c in range(nc - BRING, nc):
        b_copy(c).wait_send()
    last_copy(1).wait()
    mine = gpart[last] + glast[1]
    grecv[last] = mine
    for b in range(8):
        turned = grecv[:, b, :].T
        g_out[:, b] = jnp.where(row == 0, turned[:64], turned[64:]).reshape(8, 8, snaps)
    for dd in range(1, 8):
        energy_copy(dd).wait()
    x_energy = tree([energy[dd, :1] for dd in range(8)])
    g_energy = tree([energy[dd, 1:] for dd in (0, 2, 4, 6)])
    for dd in range(2, 8):
        last_copy(dd).wait()
    chips = [mine] + [glast[dd] + glast[dd + 1] for dd in (2, 4, 6)]
    final = jnp.sum(tree([g * g for g in chips]))
    g_energy = jnp.where(lax.broadcasted_iota(jnp.int32, (1, 128), 1) == last, final, g_energy)
    e_out[...] = ((x_energy - g_energy) / x_energy)[:, :snaps]


def finish(g_in, e_in, g_out, e_out, sem):
    copies = [pltpu.make_async_copy(g_in, g_out, sem.at[0]), pltpu.make_async_copy(e_in, e_out, sem.at[1])]
    for copy in copies:
        copy.start()
    for copy in copies:
        copy.wait()


def solution(mesh):
    rows = 32

    def local_part(x_block, f_one, f_two, f_three):
        snaps = x_block.shape[0]
        nq = 128 // rows
        nc = snaps * nq
        dma = pltpu.SemaphoreType.DMA
        hbm = pl.BlockSpec(memory_space=pltpu.HBM)
        vmem = pl.BlockSpec(memory_space=pltpu.VMEM)
        g, e = pl.pallas_call(
            functools.partial(kernel, snaps, rows),
            out_shape=(pltpu.VMEM((8, 8, 8, snaps), F32), pltpu.VMEM((1, snaps), F32)),
            in_specs=[hbm] * 4,
            out_specs=(vmem, vmem),
            scratch_shapes=[
                pltpu.VMEM((XBUF, rows * 128, 128), BF16),
                pltpu.VMEM((16, 256), F32), pltpu.VMEM((16, 256), F32), pltpu.VMEM((16, 256), F32),
                pltpu.VMEM((16, 128), BF16), pltpu.VMEM((16, 128), BF16),
                pltpu.VMEM((nq, rows * 8, 128), BF16),
                pltpu.VMEM((RING, rows, 8, 128), F32), pltpu.VMEM((RING, rows, 8, 128), F32), pltpu.VMEM((RING, rows, 8, 128), F32),
                pltpu.VMEM((BRING, 8, rows * 8), F32), pltpu.VMEM((BRING, 8, rows * 8), F32), pltpu.VMEM((BRING, 8, rows * 8), F32),
                pltpu.VMEM((snaps, 8, 128), F32), pltpu.VMEM((snaps, 8, 128), F32),
                pltpu.VMEM((snaps, 8, 128), F32), pltpu.VMEM((8, 2, 128), F32), pltpu.VMEM((8, 8, 128), F32),
                dma((XBUF,)), dma((3,)), dma((RING,)), dma((RING,)), dma((BRING,)), dma((BRING,)), dma((2,)), dma((8,)), dma((8,)), dma((8,)), dma((8,)),
            ],
            compiler_params=pltpu.CompilerParams(collective_id=0, has_side_effects=True, vmem_limit_bytes=40 * 1024 * 1024),
        )(x_block.reshape(nc, rows * 128, 128), *(pltpu.with_memory_space_constraint(f.T, pltpu.HBM) for f in (f_one, f_two, f_three)))
        g, e = pl.pallas_call(
            finish,
            out_shape=(jax.ShapeDtypeStruct((8, 8, 8, snaps), F32), jax.ShapeDtypeStruct((1, snaps), F32)),
            in_specs=[vmem] * 2,
            out_specs=(hbm, hbm),
            scratch_shapes=[dma((2,))],
            compiler_params=pltpu.CompilerParams(vmem_limit_bytes=4 * 1024 * 1024),
        )(*(pltpu.with_memory_space_constraint(r, pltpu.VMEM) for r in (g, e)))
        return g.transpose(3, 0, 1, 2), e.reshape(snaps)

    return jax.shard_map(local_part, mesh=mesh, in_specs=(P(None, 'row', 'col', 'slab'), P(None, None), P(None, None), P(None, None)), out_specs=(P(None, 'row', 'col', 'slab'), P()), check_vma=False)
```

```python
import functools

import jax
import jax.numpy as jnp
from jax import lax
from jax.experimental import pallas as pl
from jax.experimental.pallas import tpu as pltpu
from jax.sharding import PartitionSpec as P

MESH = pl.DeviceIdType.MESH
F32, BF16 = jnp.float32, jnp.bfloat16
NT = (((1,), (1,)), ((), ()))

LAG = 4
RING = 2 * LAG
XBUF = 4
BRING = 4
SUB = 8


def other(axis):
    return {axis: 1 - lax.axis_index(axis)}


def offset_peer(dd):
    peer = {}
    for bit, axis in ((4, 'slab'), (2, 'col'), (1, 'row')):
        here = lax.axis_index(axis)
        peer[axis] = 1 - here if dd & bit else here
    return peer


def tree(parts):
    while len(parts) > 1:
        parts = [parts[k] + parts[k + 1] for k in range(0, len(parts), 2)]
    return parts[0]


def kernel(snaps, rows, x_hbm, f1_hbm, f2_hbm, f3_hbm, g_out, e_out,
           xbuf, f1, f2, f3, u3w, u2w, w1, own, ysend, yrecv, bown, xsend, xrecv,
           gpart, grecv, ex, energy, glast, u2n, w1o, blast, x_sem, f_sem, ys_sem, yr_sem, xs_sem, xr_sem, g_sem, en_ssem, en_rsem, gl_ssem, gl_rsem, bl_ssem, bl_rsem, x0_sem):
    nq = 128 // rows
    nc = snaps * nq
    width = rows * 8
    last = snaps - 1
    slab, col, row = (lax.axis_index(a) for a in ('slab', 'col', 'row'))

    def x_copy(c):
        slot = lax.rem(c, XBUF)
        return pltpu.make_async_copy(x_hbm.at[c], xbuf.at[slot], x_sem.at[slot])

    f_copies = [pltpu.make_async_copy(src, dst, f_sem.at[k]) for k, (src, dst) in enumerate(((f3_hbm, f3), (f2_hbm, f2), (f1_hbm, f1)))]
    pieces = rows // SUB
    x_first = [pltpu.make_async_copy(x_hbm.at[0, pl.ds(k * SUB * 128, SUB * 128)], xbuf.at[0, pl.ds(k * SUB * 128, SUB * 128)], x0_sem.at[k]) for k in range(pieces)]
    x_first[0].start()
    f_copies[0].start()
    for copy in x_first[1:]:
        copy.start()

    barrier = pltpu.get_barrier_semaphore()
    for dd in (4, 2, 1):
        pl.semaphore_signal(barrier, inc=1, device_id=offset_peer(dd), device_id_type=MESH)

    def swapped(block, flip):
        return jnp.where(flip == 0, block, jnp.concatenate([block[8:], block[:8]], axis=0)).astype(BF16)

    f_copies[0].wait()
    u3w[...] = swapped(f3[:, pl.ds(pl.multiple_of(slab * 128, 128), 128)], slab)
    ex[...] = jnp.zeros_like(ex)

    def y_copy(c):
        slot = lax.rem(c, RING)
        return pltpu.make_async_remote_copy(ysend.at[slot], yrecv.at[slot], ys_sem.at[slot], yr_sem.at[slot], device_id=other('slab'), device_id_type=MESH)

    def b_copy(c):
        slot = lax.rem(c, BRING)
        return pltpu.make_async_remote_copy(xsend.at[slot], xrecv.at[slot], xs_sem.at[slot], xr_sem.at[slot], device_id=other('col'), device_id_type=MESH)

    def y_first(k):
        part = pl.ds(k * SUB, SUB)
        return pltpu.make_async_remote_copy(ysend.at[0, part], yrecv.at[0, part], ys_sem.at[0], yr_sem.at[0], device_id=other('slab'), device_id_type=MESH)

    def wide_copy(dd):
        return pltpu.make_async_remote_copy(blast.at[0], blast.at[dd], bl_ssem.at[dd], bl_rsem.at[dd], device_id=offset_peer(dd), device_id_type=MESH)

    def energy_copy(dd):
        return pltpu.make_async_remote_copy(energy.at[0], energy.at[dd], en_ssem.at[dd], en_rsem.at[dd], device_id=offset_peer(dd), device_id_type=MESH)

    def last_copy(dd):
        return pltpu.make_async_remote_copy(gpart.at[last], glast.at[dd], gl_ssem.at[dd], gl_rsem.at[dd], device_id=offset_peer(dd), device_id_type=MESH)

    early = pl.ds(0, last)
    g_copy = pltpu.make_async_remote_copy(gpart.at[early], grecv.at[early], g_sem.at[0], g_sem.at[1], device_id=other('row'), device_id_type=MESH)

    def block(slot, xs, k):
        x = xbuf[xs, pl.ds(pl.multiple_of(k * SUB * 128, SUB * 128), SUB * 128), :]
        part = lax.dot_general(u3w[...], x, NT, preferred_element_type=F32)
        for i in range(SUB):
            own[slot, k * SUB + i] = part[:8, i * 128:(i + 1) * 128]
            ysend[slot, k * SUB + i] = part[8:, i * 128:(i + 1) * 128]
        xf = x.astype(F32).reshape(-1, 4, 8, 128)
        return jnp.sum(xf * xf, axis=0)

    def mode_three(c):
        slot, xs = lax.rem(c, RING), lax.rem(c, XBUF)
        x_copy(c).wait()

        @pl.when(c >= RING)
        def _():
            y_copy(c).wait_send()

        acc = lax.fori_loop(0, pieces, lambda k, acc: acc + block(slot, xs, k), jnp.zeros((4, 8, 128), F32))
        t = lax.div(c, nq)
        ex[t] += jnp.sum(acc, axis=0)

        @pl.when(c + XBUF < nc)
        def _():
            x_copy(c + XBUF).start()

    def mode_two_rows(c):
        slot = lax.rem(c, RING)
        y_copy(c).wait_recv()
        return (own[slot] + yrecv[slot]).reshape(width, 128).astype(BF16)

    def mode_two(c):
        bslot = lax.rem(c, BRING)

        @pl.when(c >= BRING)
        def _():
            b_copy(c).wait_send()

        part = lax.dot_general(u2w[...], mode_two_rows(c), NT, preferred_element_type=F32)
        bown[bslot] = part[:8]
        xsend[bslot] = part[8:]
        b_copy(c).start()

    def mode_one(c):
        bslot = lax.rem(c, BRING)
        b_copy(c).wait_recv()
        b = (bown[bslot] + xrecv[bslot]).astype(BF16)
        q, t = lax.rem(c, nq), lax.div(c, nq)
        g = jnp.dot(b, w1[q], preferred_element_type=F32)

        @pl.when(q == 0)
        def _():
            gpart[t] = g

        @pl.when(q > 0)
        def _():
            gpart[t] += g

    def late_setup():
        f_copies[1].wait()
        f_copies[2].wait()
        block_two = f2[:, pl.ds(pl.multiple_of(col * 128, 128), 128)]
        u2n[...] = block_two.astype(BF16)
        u2w[...] = swapped(block_two, col)
        spread = (lax.broadcasted_iota(jnp.int32, (16, 128), 1) // 8 == lax.broadcasted_iota(jnp.int32, (16, 128), 0)).astype(BF16)
        r = lax.broadcasted_iota(jnp.int32, (width, 128), 0)
        l = lax.broadcasted_iota(jnp.int32, (width, 128), 1)

        def diagonal(which, q):
            u1 = f1[:, pl.ds(pl.multiple_of(which * 128, 128), 128)].astype(BF16)
            pick = (l == q * rows + r // 8).astype(BF16)
            rowed = lax.dot_general(pick, u1, NT, preferred_element_type=F32).astype(BF16)
            wide = jnp.dot(rowed, spread, preferred_element_type=F32)
            return jnp.where(r % 8 == l % 8, wide, 0.0).astype(BF16)

        for q in range(nq):
            w1[q] = diagonal(row, q)
        w1o[...] = diagonal(1 - row, nq - 1)

    def as_row(column, count):
        i = lax.broadcasted_iota(jnp.int32, (count, 128), 0)
        return jnp.sum(jnp.where(i == lax.broadcasted_iota(jnp.int32, (count, 128), 1), column, 0.0), axis=0, keepdims=True)

    def row_sums(blocks):
        return as_row(jnp.sum(jnp.sum(blocks, axis=1), axis=1, keepdims=True), blocks.shape[0])

    def step(s, carry):
        @pl.when((s >= 2) & (s <= nc))
        def _():
            y_copy(s - 1).start()

        @pl.when(s < nc)
        def _():
            mode_three(s)

        @pl.when(s == 2)
        def _():
            late_setup()

        @pl.when(s == nc)
        def _():
            energy[0, :1] = row_sums(ex[...])

        @pl.when(s == nc + LAG - 3)
        def _():
            g_copy.start()

        @pl.when(s >= LAG)
        def _():
            mode_two(s - LAG)

        @pl.when(s == nc + LAG - 2)
        def _():
            g_copy.wait()
            g = gpart[early] + grecv[early]
            grecv[early] = g
            energy[0, 1:] = row_sums(g * g)

        @pl.when(s >= LAG + 1)
        def _():
            mode_one(s - LAG - 1)

        return carry

    first = jnp.zeros((4, 8, 128), F32)
    for k in range(pieces):
        x_first[k].wait()
        if k == 0:
            for c in range(1, XBUF):
                x_copy(c).start()
            f_copies[1].start()
            f_copies[2].start()
        first += block(0, 0, k)
        if k == 0:
            pl.semaphore_wait(barrier, 3)
        y_first(k).start()
    ex[0] = jnp.sum(first, axis=0)
    x_copy(XBUF).start()
    lax.fori_loop(1, nc + LAG - 1, step, 0)

    for dd in range(1, 8):
        energy_copy(dd).start()
    mode_one(nc - 2)
    far_first = (6, 7, 4, 5, 2, 3, 1)
    for dd in far_first:
        last_copy(dd).start()
    blast[0] = lax.dot_general(u2n[...], mode_two_rows(nc - 1), NT, preferred_element_type=F32)
    for dd in far_first:
        wide_copy(dd).start()
    for c in range(nc - RING, nc):
        y_copy(c).wait_send()
    for c in range(nc - 1 - BRING, nc - 1):
        b_copy(c).wait_send()

    def chip_pair(base):
        b_here = (blast[base] + blast[base + 2]).astype(BF16)
        b_twin = (blast[base + 1] + blast[base + 3]).astype(BF16)
        part = jnp.dot(b_here, w1[nq - 1], preferred_element_type=F32) + jnp.dot(b_twin, w1o[...], preferred_element_type=F32)
        low, high = part[:8], part[8:]
        return jnp.where(col == 0, low, high), jnp.where(col == 0, high, low)

    last_copy(1).wait()
    for dd in (1, 2, 3):
        wide_copy(dd).wait()
    near = chip_pair(0)
    mine = (gpart[last] + glast[1]) + near[0]
    grecv[last] = mine
    for b in range(8):
        turned = grecv[:, b, :].T
        g_out[:, b] = jnp.where(row == 0, turned[:64], turned[64:]).reshape(8, 8, snaps)
    for dd in range(1, 8):
        energy_copy(dd).wait()
    x_energy = tree([energy[dd, :1] for dd in range(8)])
    g_energy = tree([energy[dd, 1:] for dd in (0, 2, 4, 6)])
    for dd in range(2, 8):
        last_copy(dd).wait()
    for dd in range(4, 8):
        wide_copy(dd).wait()
    far = chip_pair(4)
    chips = [mine] + [(glast[dd] + glast[dd + 1]) + add for dd, add in ((2, near[1]), (4, far[0]), (6, far[1]))]
    final = jnp.sum(tree([g * g for g in chips]))
    g_energy = jnp.where(lax.broadcasted_iota(jnp.int32, (1, 128), 1) == last, final, g_energy)
    e_out[...] = ((x_energy - g_energy) / x_energy)[:, :snaps]


def finish(g_in, e_in, g_out, e_out, sem):
    copies = [pltpu.make_async_copy(g_in, g_out, sem.at[0]), pltpu.make_async_copy(e_in, e_out, sem.at[1])]
    for copy in copies:
        copy.start()
    for copy in copies:
        copy.wait()


def solution(mesh):
    rows = 32

    def local_part(x_block, f_one, f_two, f_three):
        snaps = x_block.shape[0]
        nq = 128 // rows
        nc = snaps * nq
        dma = pltpu.SemaphoreType.DMA
        hbm = pl.BlockSpec(memory_space=pltpu.HBM)
        vmem = pl.BlockSpec(memory_space=pltpu.VMEM)
        g, e = pl.pallas_call(
            functools.partial(kernel, snaps, rows),
            out_shape=(pltpu.VMEM((8, 8, 8, snaps), F32), pltpu.VMEM((1, snaps), F32)),
            in_specs=[hbm] * 4,
            out_specs=(vmem, vmem),
            scratch_shapes=[
                pltpu.VMEM((XBUF, rows * 128, 128), BF16),
                pltpu.VMEM((16, 256), F32), pltpu.VMEM((16, 256), F32), pltpu.VMEM((16, 256), F32),
                pltpu.VMEM((16, 128), BF16), pltpu.VMEM((16, 128), BF16),
                pltpu.VMEM((nq, rows * 8, 128), BF16),
                pltpu.VMEM((RING, rows, 8, 128), F32), pltpu.VMEM((RING, rows, 8, 128), F32), pltpu.VMEM((RING, rows, 8, 128), F32),
                pltpu.VMEM((BRING, 8, rows * 8), F32), pltpu.VMEM((BRING, 8, rows * 8), F32), pltpu.VMEM((BRING, 8, rows * 8), F32),
                pltpu.VMEM((snaps, 8, 128), F32), pltpu.VMEM((snaps, 8, 128), F32),
                pltpu.VMEM((snaps, 8, 128), F32), pltpu.VMEM((8, 2, 128), F32), pltpu.VMEM((8, 8, 128), F32),
                pltpu.VMEM((16, 128), BF16), pltpu.VMEM((rows * 8, 128), BF16), pltpu.VMEM((8, 16, rows * 8), F32),
                dma((XBUF,)), dma((3,)), dma((RING,)), dma((RING,)), dma((BRING,)), dma((BRING,)), dma((2,)), dma((8,)), dma((8,)), dma((8,)), dma((8,)), dma((8,)), dma((8,)), dma((rows // SUB,)),
            ],
            compiler_params=pltpu.CompilerParams(collective_id=0, has_side_effects=True, vmem_limit_bytes=40 * 1024 * 1024),
        )(x_block.reshape(nc, rows * 128, 128), *(pltpu.with_memory_space_constraint(f.T, pltpu.HBM) for f in (f_one, f_two, f_three)))
        g, e = pl.pallas_call(
            finish,
            out_shape=(jax.ShapeDtypeStruct((8, 8, 8, snaps), F32), jax.ShapeDtypeStruct((1, snaps), F32)),
            in_specs=[vmem] * 2,
            out_specs=(hbm, hbm),
            scratch_shapes=[dma((2,))],
            compiler_params=pltpu.CompilerParams(vmem_limit_bytes=4 * 1024 * 1024),
        )(*(pltpu.with_memory_space_constraint(r, pltpu.VMEM) for r in (g, e)))
        return g.transpose(3, 0, 1, 2), e.reshape(snaps)

    return jax.shard_map(local_part, mesh=mesh, in_specs=(P(None, 'row', 'col', 'slab'), P(None, None), P(None, None), P(None, None)), out_specs=(P(None, 'row', 'col', 'slab'), P()), check_vma=False)
```

```python
import functools

import jax
import jax.numpy as jnp
from jax import lax
from jax.experimental import pallas as pl
from jax.experimental.pallas import tpu as pltpu
from jax.sharding import PartitionSpec as P

MESH = pl.DeviceIdType.MESH
F32, BF16 = jnp.float32, jnp.bfloat16
NT = (((1,), (1,)), ((), ()))

LAG = 3
RING = 2 * LAG
HELD = LAG + 1
XBUF = 4
BRING = 4
BHELD = 2
SUB = 8


def other(axis):
    return {axis: 1 - lax.axis_index(axis)}


def offset_peer(dd):
    peer = {}
    for bit, axis in ((4, 'slab'), (2, 'col'), (1, 'row')):
        here = lax.axis_index(axis)
        peer[axis] = 1 - here if dd & bit else here
    return peer


def tree(parts):
    while len(parts) > 1:
        parts = [parts[k] + parts[k + 1] for k in range(0, len(parts), 2)]
    return parts[0]


def kernel(snaps, rows, x_hbm, f1_hbm, f2_hbm, f3_hbm, g_out, e_out,
           xbuf, f1, f2, f3, u3w, u2w, w1, own, ysend, yrecv, bown, xsend, xrecv,
           gpart, grecv, ex, energy, glast, u2n, w1o, blast, x_sem, ys_sem, yr_sem, xs_sem, xr_sem, g_sem, all_send, all_recv):
    nq = 128 // rows
    nc = snaps * nq
    width = rows * 8
    last = snaps - 1
    slab, col, row = (lax.axis_index(a) for a in ('slab', 'col', 'row'))

    def x_copy(c):
        slot = lax.rem(c, XBUF)
        return pltpu.make_async_copy(x_hbm.at[c], xbuf.at[slot], x_sem.at[slot])

    f_copies = [pltpu.make_async_copy(src, dst, all_send.at[k]) for k, (src, dst) in enumerate(((f3_hbm, f3), (f2_hbm, f2), (f1_hbm, f1)))]
    pieces = rows // SUB
    x_first = [pltpu.make_async_copy(x_hbm.at[0, pl.ds(k * SUB * 128, SUB * 128)], xbuf.at[0, pl.ds(k * SUB * 128, SUB * 128)], x_sem.at[k]) for k in range(pieces)]
    x_first[0].start()
    f_copies[0].start()
    for copy in x_first[1:]:
        copy.start()

    barrier = pltpu.get_barrier_semaphore()
    for dd in (4, 2, 1):
        pl.semaphore_signal(barrier, inc=1, device_id=offset_peer(dd), device_id_type=MESH)

    def swapped(block, flip):
        return jnp.where(flip == 0, block, jnp.concatenate([block[8:], block[:8]], axis=0)).astype(BF16)

    f_copies[0].wait()
    u3w[...] = swapped(f3[:, pl.ds(pl.multiple_of(slab * 128, 128), 128)], slab)
    ex[...] = jnp.zeros_like(ex)

    def y_copy(c):
        held, slot = lax.rem(c, HELD), lax.rem(c, RING)
        return pltpu.make_async_remote_copy(ysend.at[held], yrecv.at[slot], ys_sem.at[lax.rem(c, LAG)], yr_sem.at[slot], device_id=other('slab'), device_id_type=MESH)

    def b_copy(c):
        held, slot = lax.rem(c, BHELD), lax.rem(c, BRING)
        return pltpu.make_async_remote_copy(xsend.at[held], xrecv.at[slot], xs_sem.at[held], xr_sem.at[slot], device_id=other('col'), device_id_type=MESH)

    def y_first(k):
        part = pl.ds(k * SUB, SUB)
        return pltpu.make_async_remote_copy(ysend.at[0, part], yrecv.at[0, part], ys_sem.at[0], yr_sem.at[0], device_id=other('slab'), device_id_type=MESH)

    def wide_copy(dd):
        return pltpu.make_async_remote_copy(blast.at[0], blast.at[dd], all_send.at[0], all_recv.at[dd // 4], device_id=offset_peer(dd), device_id_type=MESH)

    def energy_copy(dd):
        return pltpu.make_async_remote_copy(energy.at[0], energy.at[dd], all_send.at[2], all_recv.at[4], device_id=offset_peer(dd), device_id_type=MESH)

    def last_copy(dd):
        return pltpu.make_async_remote_copy(gpart.at[last], glast.at[dd], all_send.at[1], all_recv.at[2 + dd // 4], device_id=offset_peer(dd), device_id_type=MESH)

    def wait_all(buffer, begin, end, sem):
        part = buffer.at[pl.ds(begin, end - begin)]
        pltpu.make_async_copy(part, part, sem).wait()

    early = pl.ds(0, last)
    g_copy = pltpu.make_async_remote_copy(gpart.at[early], grecv.at[early], all_send.at[2], g_sem.at[0], device_id=other('row'), device_id_type=MESH)

    def block(slot, xs, k):
        x = xbuf[xs, pl.ds(pl.multiple_of(k * SUB * 128, SUB * 128), SUB * 128), :]
        part = lax.dot_general(u3w[...], x, NT, preferred_element_type=F32)
        for i in range(SUB):
            own[slot, k * SUB + i] = part[:8, i * 128:(i + 1) * 128]
            ysend[slot, k * SUB + i] = part[8:, i * 128:(i + 1) * 128]
        xf = x.astype(F32).reshape(-1, 4, 8, 128)
        return jnp.sum(xf * xf, axis=0)

    def mode_three(c):
        slot, xs = lax.rem(c, HELD), lax.rem(c, XBUF)
        x_copy(c).wait()
        acc = lax.fori_loop(0, pieces, lambda k, acc: acc + block(slot, xs, k), jnp.zeros((4, 8, 128), F32))
        t = lax.div(c, nq)
        ex[t] += jnp.sum(acc, axis=0)

        @pl.when(c + XBUF < nc)
        def _():
            x_copy(c + XBUF).start()

    def mode_two_rows(c):
        y_copy(c).wait_recv()
        return (own[lax.rem(c, HELD)] + yrecv[lax.rem(c, RING)]).reshape(width, 128).astype(BF16)

    def mode_two(c):
        bslot = lax.rem(c, BHELD)

        @pl.when(c >= BHELD)
        def _():
            b_copy(c).wait_send()

        part = lax.dot_general(u2w[...], mode_two_rows(c), NT, preferred_element_type=F32)
        bown[bslot] = part[:8]
        xsend[bslot] = part[8:]
        b_copy(c).start()

    def mode_one(c):
        b_copy(c).wait_recv()
        b = (bown[lax.rem(c, BHELD)] + xrecv[lax.rem(c, BRING)]).astype(BF16)
        q, t = lax.rem(c, nq), lax.div(c, nq)
        g = jnp.dot(b, w1[q], preferred_element_type=F32)

        @pl.when(q == 0)
        def _():
            gpart[t] = g

        @pl.when(q > 0)
        def _():
            gpart[t] += g

    def late_setup():
        f_copies[1].wait()
        f_copies[2].wait()
        block_two = f2[:, pl.ds(pl.multiple_of(col * 128, 128), 128)]
        u2n[...] = block_two.astype(BF16)
        u2w[...] = swapped(block_two, col)
        spread = (lax.broadcasted_iota(jnp.int32, (16, 128), 1) // 8 == lax.broadcasted_iota(jnp.int32, (16, 128), 0)).astype(BF16)
        r = lax.broadcasted_iota(jnp.int32, (width, 128), 0)
        l = lax.broadcasted_iota(jnp.int32, (width, 128), 1)

        def diagonal(which, q):
            u1 = f1[:, pl.ds(pl.multiple_of(which * 128, 128), 128)].astype(BF16)
            pick = (l == q * rows + r // 8).astype(BF16)
            rowed = lax.dot_general(pick, u1, NT, preferred_element_type=F32).astype(BF16)
            wide = jnp.dot(rowed, spread, preferred_element_type=F32)
            return jnp.where(r % 8 == l % 8, wide, 0.0).astype(BF16)

        for q in range(nq):
            w1[q] = diagonal(row, q)
        w1o[...] = diagonal(1 - row, nq - 1)

    def as_row(column, count):
        i = lax.broadcasted_iota(jnp.int32, (count, 128), 0)
        return jnp.sum(jnp.where(i == lax.broadcasted_iota(jnp.int32, (count, 128), 1), column, 0.0), axis=0, keepdims=True)

    def row_sums(blocks):
        return as_row(jnp.sum(jnp.sum(blocks, axis=1), axis=1, keepdims=True), blocks.shape[0])

    def step(s, carry):
        @pl.when((s > LAG) & (s <= nc))
        def _():
            y_copy(s - 1 - LAG).wait_send()

        @pl.when((s >= 2) & (s <= nc))
        def _():
            y_copy(s - 1).start()

        @pl.when(s < nc)
        def _():
            mode_three(s)

        @pl.when(s == 2)
        def _():
            late_setup()

        @pl.when(s == nc)
        def _():
            energy[0, :1] = row_sums(ex[...])

        @pl.when(s == nc + LAG - 3)
        def _():
            g_copy.start()

        @pl.when(s >= LAG)
        def _():
            mode_two(s - LAG)

        @pl.when(s == nc + LAG - 2)
        def _():
            g_copy.wait()
            g = gpart[early] + grecv[early]
            grecv[early] = g
            energy[0, 1:] = row_sums(g * g)

        @pl.when(s >= LAG + 1)
        def _():
            mode_one(s - LAG - 1)

        return carry

    first = jnp.zeros((4, 8, 128), F32)
    for k in range(pieces):
        x_first[k].wait()
        if k == 0:
            f_copies[1].start()
            f_copies[2].start()
        else:
            x_copy(k).start()
        first += block(0, 0, k)
        if k == 0:
            pl.semaphore_wait(barrier, 3)
        y_first(k).start()
    ex[0] = jnp.sum(first, axis=0)
    x_copy(XBUF).start()
    lax.fori_loop(1, nc + LAG - 1, step, 0)

    for dd in range(1, 8):
        energy_copy(dd).start()
    mode_one(nc - 2)
    far_first = (6, 7, 4, 5, 2, 3, 1)
    for dd in far_first:
        last_copy(dd).start()
    blast[0] = lax.dot_general(u2n[...], mode_two_rows(nc - 1), NT, preferred_element_type=F32)
    for dd in far_first:
        wide_copy(dd).start()
    for c in range(nc - LAG, nc):
        y_copy(c).wait_send()
    for c in range(nc - 1 - BHELD, nc - 1):
        b_copy(c).wait_send()
    wait_all(energy, 1, 8, all_send.at[2])
    wait_all(glast, 1, 8, all_send.at[1])

    def chip_pair(base):
        b_here = (blast[base] + blast[base + 2]).astype(BF16)
        b_twin = (blast[base + 1] + blast[base + 3]).astype(BF16)
        part = jnp.dot(b_here, w1[nq - 1], preferred_element_type=F32) + jnp.dot(b_twin, w1o[...], preferred_element_type=F32)
        low, high = part[:8], part[8:]
        return jnp.where(col == 0, low, high), jnp.where(col == 0, high, low)

    wait_all(glast, 1, 4, all_recv.at[2])
    wait_all(blast, 1, 4, all_recv.at[0])
    near = chip_pair(0)
    mine = (gpart[last] + glast[1]) + near[0]
    grecv[last] = mine
    for b in range(8):
        turned = grecv[:, b, :].T
        g_out[:, b] = jnp.where(row == 0, turned[:64], turned[64:]).reshape(8, 8, snaps)
    wait_all(energy, 1, 8, all_recv.at[4])
    x_energy = tree([energy[dd, :1] for dd in range(8)])
    g_energy = tree([energy[dd, 1:] for dd in (0, 2, 4, 6)])
    wait_all(blast, 1, 8, all_send.at[0])
    wait_all(glast, 4, 8, all_recv.at[3])
    wait_all(blast, 4, 8, all_recv.at[1])
    far = chip_pair(4)
    chips = [mine] + [(glast[dd] + glast[dd + 1]) + add for dd, add in ((2, near[1]), (4, far[0]), (6, far[1]))]
    final = jnp.sum(tree([g * g for g in chips]))
    g_energy = jnp.where(lax.broadcasted_iota(jnp.int32, (1, 128), 1) == last, final, g_energy)
    e_out[...] = ((x_energy - g_energy) / x_energy)[:, :snaps]


def finish(g_in, e_in, g_out, e_out, sem):
    copies = [pltpu.make_async_copy(g_in, g_out, sem.at[0]), pltpu.make_async_copy(e_in, e_out, sem.at[1])]
    for copy in copies:
        copy.start()
    for copy in copies:
        copy.wait()


def solution(mesh):
    rows = 32

    def local_part(x_block, f_one, f_two, f_three):
        snaps = x_block.shape[0]
        nq = 128 // rows
        nc = snaps * nq
        dma = pltpu.SemaphoreType.DMA
        hbm = pl.BlockSpec(memory_space=pltpu.HBM)
        vmem = pl.BlockSpec(memory_space=pltpu.VMEM)
        g, e = pl.pallas_call(
            functools.partial(kernel, snaps, rows),
            out_shape=(pltpu.VMEM((8, 8, 8, snaps), F32), pltpu.VMEM((1, snaps), F32)),
            in_specs=[hbm] * 4,
            out_specs=(vmem, vmem),
            scratch_shapes=[
                pltpu.VMEM((XBUF, rows * 128, 128), BF16),
                pltpu.VMEM((16, 256), F32), pltpu.VMEM((16, 256), F32), pltpu.VMEM((16, 256), F32),
                pltpu.VMEM((16, 128), BF16), pltpu.VMEM((16, 128), BF16),
                pltpu.VMEM((nq, rows * 8, 128), BF16),
                pltpu.VMEM((HELD, rows, 8, 128), F32), pltpu.VMEM((HELD, rows, 8, 128), F32), pltpu.VMEM((RING, rows, 8, 128), F32),
                pltpu.VMEM((BHELD, 8, rows * 8), F32), pltpu.VMEM((BHELD, 8, rows * 8), F32), pltpu.VMEM((BRING, 8, rows * 8), F32),
                pltpu.VMEM((snaps, 8, 128), F32), pltpu.VMEM((snaps, 8, 128), F32),
                pltpu.VMEM((snaps, 8, 128), F32), pltpu.VMEM((8, 2, 128), F32), pltpu.VMEM((8, 8, 128), F32),
                pltpu.VMEM((16, 128), BF16), pltpu.VMEM((rows * 8, 128), BF16), pltpu.VMEM((8, 16, rows * 8), F32),
                dma((XBUF,)), dma((LAG,)), dma((RING,)), dma((BHELD,)), dma((BRING,)), dma((1,)), dma((3,)), dma((5,)),
            ],
            compiler_params=pltpu.CompilerParams(collective_id=0, has_side_effects=True, vmem_limit_bytes=40 * 1024 * 1024),
        )(x_block.reshape(nc, rows * 128, 128), *(pltpu.with_memory_space_constraint(f.T, pltpu.HBM) for f in (f_one, f_two, f_three)))
        g, e = pl.pallas_call(
            finish,
            out_shape=(jax.ShapeDtypeStruct((8, 8, 8, snaps), F32), jax.ShapeDtypeStruct((1, snaps), F32)),
            in_specs=[vmem] * 2,
            out_specs=(hbm, hbm),
            scratch_shapes=[dma((2,))],
            compiler_params=pltpu.CompilerParams(vmem_limit_bytes=4 * 1024 * 1024),
        )(*(pltpu.with_memory_space_constraint(r, pltpu.VMEM) for r in (g, e)))
        return g.transpose(3, 0, 1, 2), e.reshape(snaps)

    return jax.shard_map(local_part, mesh=mesh, in_specs=(P(None, 'row', 'col', 'slab'), P(None, None), P(None, None), P(None, None)), out_specs=(P(None, 'row', 'col', 'slab'), P()), check_vma=False)
```

```python
import functools

import jax
import jax.numpy as jnp
from jax import lax
from jax.experimental import pallas as pl
from jax.experimental.pallas import tpu as pltpu
from jax.sharding import PartitionSpec as P

MESH = pl.DeviceIdType.MESH
F32, BF16 = jnp.float32, jnp.bfloat16
NT = (((1,), (1,)), ((), ()))

LAG = 3
RING = 2 * LAG
HELD = LAG + 1
XBUF = 4
BRING = 4
BHELD = 2
SUB = 8
LAST = 2


def other(axis):
    return {axis: 1 - lax.axis_index(axis)}


def offset_peer(dd):
    peer = {}
    for bit, axis in ((4, 'slab'), (2, 'col'), (1, 'row')):
        here = lax.axis_index(axis)
        peer[axis] = 1 - here if dd & bit else here
    return peer


def tree(parts):
    while len(parts) > 1:
        parts = [parts[k] + parts[k + 1] for k in range(0, len(parts), 2)]
    return parts[0]


def kernel(snaps, rows, x_hbm, f1_hbm, f2_hbm, f3_hbm, g_out, e_out,
           xbuf, f1, f2, f3, u3w, u2w, w1, own, ysend, yrecv, bown, xsend, xrecv,
           gpart, grecv, ex, energy, glast, u2n, w1o, blast, x_sem, ys_sem, yr_sem, xs_sem, xr_sem, g_sem, all_send, all_recv, yls_sem, ylr_sem):
    nq = 128 // rows
    nc = snaps * nq
    width = rows * 8
    last = snaps - 1
    slab, col, row = (lax.axis_index(a) for a in ('slab', 'col', 'row'))

    def x_copy(c):
        slot = lax.rem(c, XBUF)
        return pltpu.make_async_copy(x_hbm.at[c], xbuf.at[slot], x_sem.at[slot])

    f_copies = [pltpu.make_async_copy(src, dst, all_send.at[k]) for k, (src, dst) in enumerate(((f3_hbm, f3), (f2_hbm, f2), (f1_hbm, f1)))]
    pieces = rows // SUB
    x_first = [pltpu.make_async_copy(x_hbm.at[0, pl.ds(k * SUB * 128, SUB * 128)], xbuf.at[0, pl.ds(k * SUB * 128, SUB * 128)], x_sem.at[k]) for k in range(pieces)]
    x_first[0].start()
    f_copies[0].start()
    for copy in x_first[1:]:
        copy.start()

    barrier = pltpu.get_barrier_semaphore()
    for dd in (4, 2, 1):
        pl.semaphore_signal(barrier, inc=1, device_id=offset_peer(dd), device_id_type=MESH)

    def swapped(block, flip):
        return jnp.where(flip == 0, block, jnp.concatenate([block[8:], block[:8]], axis=0)).astype(BF16)

    f_copies[0].wait()
    u3w[...] = swapped(f3[:, pl.ds(pl.multiple_of(slab * 128, 128), 128)], slab)
    ex[...] = jnp.zeros_like(ex)

    def y_copy(c):
        held, slot = lax.rem(c, HELD), lax.rem(c, RING)
        return pltpu.make_async_remote_copy(ysend.at[held], yrecv.at[slot], ys_sem.at[lax.rem(c, LAG)], yr_sem.at[slot], device_id=other('slab'), device_id_type=MESH)

    def b_copy(c):
        held, slot = lax.rem(c, BHELD), lax.rem(c, BRING)
        return pltpu.make_async_remote_copy(xsend.at[held], xrecv.at[slot], xs_sem.at[held], xr_sem.at[slot], device_id=other('col'), device_id_type=MESH)

    def y_first(k):
        part = pl.ds(k * SUB, SUB)
        return pltpu.make_async_remote_copy(ysend.at[0, part], yrecv.at[0, part], ys_sem.at[0], yr_sem.at[0], device_id=other('slab'), device_id_type=MESH)

    def y_last(k):
        part = pl.ds(k * (rows // LAST), rows // LAST)
        return pltpu.make_async_remote_copy(ysend.at[(nc - 1) % HELD, part], yrecv.at[(nc - 1) % RING, part], yls_sem.at[0], ylr_sem.at[k], device_id=other('slab'), device_id_type=MESH)

    def wide_copy(dd, k):
        return pltpu.make_async_remote_copy(blast.at[0, k], blast.at[dd, k], all_send.at[0], all_recv.at[dd // 4], device_id=offset_peer(dd), device_id_type=MESH)

    def energy_copy(dd):
        return pltpu.make_async_remote_copy(energy.at[0], energy.at[dd], all_send.at[2], all_recv.at[4], device_id=offset_peer(dd), device_id_type=MESH)

    def last_copy(dd):
        return pltpu.make_async_remote_copy(gpart.at[last], glast.at[dd], all_send.at[1], all_recv.at[2 + dd // 4], device_id=offset_peer(dd), device_id_type=MESH)

    def wait_all(buffer, begin, end, sem):
        part = buffer.at[pl.ds(begin, end - begin)]
        pltpu.make_async_copy(part, part, sem).wait()

    early = pl.ds(0, last)
    g_copy = pltpu.make_async_remote_copy(gpart.at[early], grecv.at[early], all_send.at[2], g_sem.at[0], device_id=other('row'), device_id_type=MESH)

    def block(slot, xs, k):
        x = xbuf[xs, pl.ds(pl.multiple_of(k * SUB * 128, SUB * 128), SUB * 128), :]
        part = lax.dot_general(u3w[...], x, NT, preferred_element_type=F32)
        for i in range(SUB):
            own[slot, k * SUB + i] = part[:8, i * 128:(i + 1) * 128]
            ysend[slot, k * SUB + i] = part[8:, i * 128:(i + 1) * 128]
        xf = x.astype(F32).reshape(-1, 4, 8, 128)
        return jnp.sum(xf * xf, axis=0)

    def mode_three(c):
        slot, xs = lax.rem(c, HELD), lax.rem(c, XBUF)
        x_copy(c).wait()
        acc = lax.fori_loop(0, pieces, lambda k, acc: acc + block(slot, xs, k), jnp.zeros((4, 8, 128), F32))
        t = lax.div(c, nq)
        ex[t] += jnp.sum(acc, axis=0)

        @pl.when(c + XBUF < nc)
        def _():
            x_copy(c + XBUF).start()

    def mode_two(c):
        bslot = lax.rem(c, BHELD)

        @pl.when(c >= BHELD)
        def _():
            b_copy(c).wait_send()

        y_copy(c).wait_recv()
        a = (own[lax.rem(c, HELD)] + yrecv[lax.rem(c, RING)]).reshape(width, 128).astype(BF16)
        part = lax.dot_general(u2w[...], a, NT, preferred_element_type=F32)
        bown[bslot] = part[:8]
        xsend[bslot] = part[8:]
        b_copy(c).start()

    def mode_one(c):
        b_copy(c).wait_recv()
        b = (bown[lax.rem(c, BHELD)] + xrecv[lax.rem(c, BRING)]).astype(BF16)
        q, t = lax.rem(c, nq), lax.div(c, nq)
        g = jnp.dot(b, w1[q], preferred_element_type=F32)

        @pl.when(q == 0)
        def _():
            gpart[t] = g

        @pl.when(q > 0)
        def _():
            gpart[t] += g

    def late_setup():
        f_copies[1].wait()
        f_copies[2].wait()
        block_two = f2[:, pl.ds(pl.multiple_of(col * 128, 128), 128)]
        u2n[...] = block_two.astype(BF16)
        u2w[...] = swapped(block_two, col)
        spread = (lax.broadcasted_iota(jnp.int32, (16, 128), 1) // 8 == lax.broadcasted_iota(jnp.int32, (16, 128), 0)).astype(BF16)
        r = lax.broadcasted_iota(jnp.int32, (width, 128), 0)
        l = lax.broadcasted_iota(jnp.int32, (width, 128), 1)

        def diagonal(which, q):
            u1 = f1[:, pl.ds(pl.multiple_of(which * 128, 128), 128)].astype(BF16)
            pick = (l == q * rows + r // 8).astype(BF16)
            rowed = lax.dot_general(pick, u1, NT, preferred_element_type=F32).astype(BF16)
            wide = jnp.dot(rowed, spread, preferred_element_type=F32)
            return jnp.where(r % 8 == l % 8, wide, 0.0).astype(BF16)

        for q in range(nq):
            w1[q] = diagonal(row, q)
        w1o[...] = diagonal(1 - row, nq - 1)

    def as_row(column, count):
        i = lax.broadcasted_iota(jnp.int32, (count, 128), 0)
        return jnp.sum(jnp.where(i == lax.broadcasted_iota(jnp.int32, (count, 128), 1), column, 0.0), axis=0, keepdims=True)

    def row_sums(blocks):
        return as_row(jnp.sum(jnp.sum(blocks, axis=1), axis=1, keepdims=True), blocks.shape[0])

    def step(s, carry):
        @pl.when((s > LAG) & (s <= nc))
        def _():
            y_copy(s - 1 - LAG).wait_send()

        @pl.when((s >= 2) & (s < nc))
        def _():
            y_copy(s - 1).start()

        @pl.when(s == nc)
        def _():
            for k in range(LAST):
                y_last(k).start()

        @pl.when(s < nc)
        def _():
            mode_three(s)

        @pl.when(s == 2)
        def _():
            late_setup()

        @pl.when(s == nc)
        def _():
            energy[0, :1] = row_sums(ex[...])

        @pl.when(s == nc + LAG - 3)
        def _():
            g_copy.start()

        @pl.when(s >= LAG)
        def _():
            mode_two(s - LAG)

        @pl.when(s == nc + LAG - 2)
        def _():
            g_copy.wait()
            g = gpart[early] + grecv[early]
            grecv[early] = g
            energy[0, 1:] = row_sums(g * g)

        @pl.when(s >= LAG + 1)
        def _():
            mode_one(s - LAG - 1)

        return carry

    first = jnp.zeros((4, 8, 128), F32)
    for k in range(pieces):
        x_first[k].wait()
        if k == 0:
            f_copies[1].start()
            f_copies[2].start()
        else:
            x_copy(k).start()
        first += block(0, 0, k)
        if k == 0:
            pl.semaphore_wait(barrier, 3)
        y_first(k).start()
    ex[0] = jnp.sum(first, axis=0)
    x_copy(XBUF).start()
    lax.fori_loop(1, nc + LAG - 1, step, 0)

    for dd in range(1, 8):
        energy_copy(dd).start()
    far_first = (6, 7, 4, 5, 2, 3, 1)
    for k in range(LAST):
        if k == LAST - 1:
            mode_one(nc - 2)
            for dd in far_first:
                last_copy(dd).start()
        y_last(k).wait_recv()
        part = pl.ds(k * (rows // LAST), rows // LAST)
        a = (own[(nc - 1) % HELD, part] + yrecv[(nc - 1) % RING, part]).reshape(width // LAST, 128).astype(BF16)
        blast[0, k] = lax.dot_general(u2n[...], a, NT, preferred_element_type=F32)
        for dd in far_first:
            wide_copy(dd, k).start()
    for c in range(nc - LAG, nc - 1):
        y_copy(c).wait_send()
    tail = ysend.at[(nc - 1) % HELD]
    pltpu.make_async_copy(tail, tail, yls_sem.at[0]).wait()
    for c in range(nc - 1 - BHELD, nc - 1):
        b_copy(c).wait_send()
    wait_all(energy, 1, 8, all_send.at[2])
    wait_all(glast, 1, 8, all_send.at[1])

    def chip_pair(base):
        def summed(first):
            return jnp.concatenate([blast[first, k] + blast[first + 2, k] for k in range(LAST)], axis=1).astype(BF16)

        b_here, b_twin = summed(base), summed(base + 1)
        part = jnp.dot(b_here, w1[nq - 1], preferred_element_type=F32) + jnp.dot(b_twin, w1o[...], preferred_element_type=F32)
        low, high = part[:8], part[8:]
        return jnp.where(col == 0, low, high), jnp.where(col == 0, high, low)

    wait_all(glast, 1, 4, all_recv.at[2])
    wait_all(blast, 1, 4, all_recv.at[0])
    near = chip_pair(0)
    mine = (gpart[last] + glast[1]) + near[0]
    grecv[last] = mine
    for b in range(8):
        turned = grecv[:, b, :].T
        g_out[:, b] = jnp.where(row == 0, turned[:64], turned[64:]).reshape(8, 8, snaps)
    wait_all(energy, 1, 8, all_recv.at[4])
    x_energy = tree([energy[dd, :1] for dd in range(8)])
    g_energy = tree([energy[dd, 1:] for dd in (0, 2, 4, 6)])
    wait_all(blast, 1, 8, all_send.at[0])
    wait_all(glast, 4, 8, all_recv.at[3])
    wait_all(blast, 4, 8, all_recv.at[1])
    far = chip_pair(4)
    chips = [mine] + [(glast[dd] + glast[dd + 1]) + add for dd, add in ((2, near[1]), (4, far[0]), (6, far[1]))]
    final = jnp.sum(tree([g * g for g in chips]))
    g_energy = jnp.where(lax.broadcasted_iota(jnp.int32, (1, 128), 1) == last, final, g_energy)
    e_out[...] = ((x_energy - g_energy) / x_energy)[:, :snaps]


def finish(g_in, e_in, g_out, e_out, sem):
    copies = [pltpu.make_async_copy(g_in, g_out, sem.at[0]), pltpu.make_async_copy(e_in, e_out, sem.at[1])]
    for copy in copies:
        copy.start()
    for copy in copies:
        copy.wait()


def solution(mesh):
    rows = 32

    def local_part(x_block, f_one, f_two, f_three):
        snaps = x_block.shape[0]
        nq = 128 // rows
        nc = snaps * nq
        dma = pltpu.SemaphoreType.DMA
        hbm = pl.BlockSpec(memory_space=pltpu.HBM)
        vmem = pl.BlockSpec(memory_space=pltpu.VMEM)
        g, e = pl.pallas_call(
            functools.partial(kernel, snaps, rows),
            out_shape=(pltpu.VMEM((8, 8, 8, snaps), F32), pltpu.VMEM((1, snaps), F32)),
            in_specs=[hbm] * 4,
            out_specs=(vmem, vmem),
            scratch_shapes=[
                pltpu.VMEM((XBUF, rows * 128, 128), BF16),
                pltpu.VMEM((16, 256), F32), pltpu.VMEM((16, 256), F32), pltpu.VMEM((16, 256), F32),
                pltpu.VMEM((16, 128), BF16), pltpu.VMEM((16, 128), BF16),
                pltpu.VMEM((nq, rows * 8, 128), BF16),
                pltpu.VMEM((HELD, rows, 8, 128), F32), pltpu.VMEM((HELD, rows, 8, 128), F32), pltpu.VMEM((RING, rows, 8, 128), F32),
                pltpu.VMEM((BHELD, 8, rows * 8), F32), pltpu.VMEM((BHELD, 8, rows * 8), F32), pltpu.VMEM((BRING, 8, rows * 8), F32),
                pltpu.VMEM((snaps, 8, 128), F32), pltpu.VMEM((snaps, 8, 128), F32),
                pltpu.VMEM((snaps, 8, 128), F32), pltpu.VMEM((8, 2, 128), F32), pltpu.VMEM((8, 8, 128), F32),
                pltpu.VMEM((16, 128), BF16), pltpu.VMEM((rows * 8, 128), BF16), pltpu.VMEM((8, LAST, 16, rows * 8 // LAST), F32),
                dma((XBUF,)), dma((LAG,)), dma((RING,)), dma((BHELD,)), dma((BRING,)), dma((1,)), dma((3,)), dma((5,)), dma((1,)), dma((LAST,)),
            ],
            compiler_params=pltpu.CompilerParams(collective_id=0, has_side_effects=True, vmem_limit_bytes=40 * 1024 * 1024),
        )(x_block.reshape(nc, rows * 128, 128), *(pltpu.with_memory_space_constraint(f.T, pltpu.HBM) for f in (f_one, f_two, f_three)))
        g, e = pl.pallas_call(
            finish,
            out_shape=(jax.ShapeDtypeStruct((8, 8, 8, snaps), F32), jax.ShapeDtypeStruct((1, snaps), F32)),
            in_specs=[vmem] * 2,
            out_specs=(hbm, hbm),
            scratch_shapes=[dma((2,))],
            compiler_params=pltpu.CompilerParams(vmem_limit_bytes=4 * 1024 * 1024),
        )(*(pltpu.with_memory_space_constraint(r, pltpu.VMEM) for r in (g, e)))
        return g.transpose(3, 0, 1, 2), e.reshape(snaps)

    return jax.shard_map(local_part, mesh=mesh, in_specs=(P(None, 'row', 'col', 'slab'), P(None, None), P(None, None), P(None, None)), out_specs=(P(None, 'row', 'col', 'slab'), P()), check_vma=False)
```

```python
import functools

import jax
import jax.numpy as jnp
from jax import lax
from jax.experimental import pallas as pl
from jax.experimental.pallas import tpu as pltpu
from jax.sharding import PartitionSpec as P

MESH = pl.DeviceIdType.MESH
F32, BF16 = jnp.float32, jnp.bfloat16
NT = (((1,), (1,)), ((), ()))

LAG = 2
RING = 2 * LAG
HELD = LAG + 1
XBUF = 3
BRING = 4
BHELD = 2
SUB = 8
LAST = 4


def other(axis):
    return {axis: 1 - lax.axis_index(axis)}


def offset_peer(dd):
    peer = {}
    for bit, axis in ((4, 'slab'), (2, 'col'), (1, 'row')):
        here = lax.axis_index(axis)
        peer[axis] = 1 - here if dd & bit else here
    return peer


def tree(parts):
    while len(parts) > 1:
        parts = [parts[k] + parts[k + 1] for k in range(0, len(parts), 2)]
    return parts[0]


def kernel(snaps, rows, x_hbm, f1_hbm, f2_hbm, f3_hbm, g_out, e_out,
           xbuf, f1, f2, f3, u3w, u2w, w1, own, ysend, yrecv, bown, xsend, xrecv,
           gpart, grecv, ex, energy, glast, u2n, w1o, blast, x_sem, ys_sem, yr_sem, xs_sem, xr_sem, g_sem, all_send, all_recv, yls_sem, ylr_sem):
    nq = 128 // rows
    nc = snaps * nq
    width = rows * 8
    last = snaps - 1
    slab, col, row = (lax.axis_index(a) for a in ('slab', 'col', 'row'))

    def x_copy(c):
        slot = lax.rem(c, XBUF)
        return pltpu.make_async_copy(x_hbm.at[c], xbuf.at[slot], x_sem.at[slot])

    f_copies = [pltpu.make_async_copy(src, dst, all_send.at[k]) for k, (src, dst) in enumerate(((f3_hbm, f3), (f2_hbm, f2), (f1_hbm, f1)))]
    pieces = rows // SUB
    x_first = [pltpu.make_async_copy(x_hbm.at[0, pl.ds(k * SUB * 128, SUB * 128)], xbuf.at[0, pl.ds(k * SUB * 128, SUB * 128)], x_sem.at[k]) for k in range(pieces)]
    x_first[0].start()
    f_copies[0].start()
    for copy in x_first[1:]:
        copy.start()

    barrier = pltpu.get_barrier_semaphore()
    for dd in (4, 2, 1):
        pl.semaphore_signal(barrier, inc=1, device_id=offset_peer(dd), device_id_type=MESH)

    def swapped(block, flip):
        return jnp.where(flip == 0, block, jnp.concatenate([block[8:], block[:8]], axis=0)).astype(BF16)

    f_copies[0].wait()
    u3w[...] = swapped(f3[:, pl.ds(pl.multiple_of(slab * 128, 128), 128)], slab)
    ex[...] = jnp.zeros_like(ex)

    def y_copy(c):
        held, slot = lax.rem(c, HELD), lax.rem(c, RING)
        return pltpu.make_async_remote_copy(ysend.at[held], yrecv.at[slot], ys_sem.at[lax.rem(c, LAG)], yr_sem.at[slot], device_id=other('slab'), device_id_type=MESH)

    def b_copy(c):
        held, slot = lax.rem(c, BHELD), lax.rem(c, BRING)
        return pltpu.make_async_remote_copy(xsend.at[held], xrecv.at[slot], xs_sem.at[held], xr_sem.at[slot], device_id=other('col'), device_id_type=MESH)

    def y_first(k):
        part = pl.ds(k * SUB, SUB)
        return pltpu.make_async_remote_copy(ysend.at[0, part], yrecv.at[0, part], ys_sem.at[0], yr_sem.at[0], device_id=other('slab'), device_id_type=MESH)

    def y_last(k):
        part = pl.ds(k * (rows // LAST), rows // LAST)
        return pltpu.make_async_remote_copy(ysend.at[(nc - 1) % HELD, part], yrecv.at[(nc - 1) % RING, part], yls_sem.at[0], ylr_sem.at[k], device_id=other('slab'), device_id_type=MESH)

    def wide_copy(dd, k):
        return pltpu.make_async_remote_copy(blast.at[0, k], blast.at[dd, k], all_send.at[0], all_recv.at[dd // 4], device_id=offset_peer(dd), device_id_type=MESH)

    def energy_copy(dd):
        return pltpu.make_async_remote_copy(energy.at[0], energy.at[dd], all_send.at[2], all_recv.at[4], device_id=offset_peer(dd), device_id_type=MESH)

    def last_copy(dd):
        return pltpu.make_async_remote_copy(gpart.at[last], glast.at[dd], all_send.at[1], all_recv.at[2 + dd // 4], device_id=offset_peer(dd), device_id_type=MESH)

    def wait_all(buffer, begin, end, sem):
        part = buffer.at[pl.ds(begin, end - begin)]
        pltpu.make_async_copy(part, part, sem).wait()

    early = pl.ds(0, last)
    g_copy = pltpu.make_async_remote_copy(gpart.at[early], grecv.at[early], all_send.at[2], g_sem.at[0], device_id=other('row'), device_id_type=MESH)

    def block(slot, xs, k):
        x = xbuf[xs, pl.ds(pl.multiple_of(k * SUB * 128, SUB * 128), SUB * 128), :]
        part = lax.dot_general(u3w[...], x, NT, preferred_element_type=F32)
        for i in range(SUB):
            own[slot, k * SUB + i] = part[:8, i * 128:(i + 1) * 128]
            ysend[slot, k * SUB + i] = part[8:, i * 128:(i + 1) * 128]
        xf = x.astype(F32).reshape(-1, 4, 8, 128)
        return jnp.sum(xf * xf, axis=0)

    def mode_three(c):
        slot, xs = lax.rem(c, HELD), lax.rem(c, XBUF)
        x_copy(c).wait()
        acc = lax.fori_loop(0, pieces, lambda k, acc: acc + block(slot, xs, k), jnp.zeros((4, 8, 128), F32))
        t = lax.div(c, nq)
        ex[t] += jnp.sum(acc, axis=0)

        @pl.when(c + XBUF < nc)
        def _():
            x_copy(c + XBUF).start()

    def mode_two(c):
        bslot = lax.rem(c, BHELD)

        @pl.when(c >= BHELD)
        def _():
            b_copy(c).wait_send()

        y_copy(c).wait_recv()
        a = (own[lax.rem(c, HELD)] + yrecv[lax.rem(c, RING)]).reshape(width, 128).astype(BF16)
        part = lax.dot_general(u2w[...], a, NT, preferred_element_type=F32)
        bown[bslot] = part[:8]
        xsend[bslot] = part[8:]
        b_copy(c).start()

    def mode_one(c):
        b_copy(c).wait_recv()
        b = (bown[lax.rem(c, BHELD)] + xrecv[lax.rem(c, BRING)]).astype(BF16)
        q, t = lax.rem(c, nq), lax.div(c, nq)
        g = jnp.dot(b, w1[q], preferred_element_type=F32)

        @pl.when(q == 0)
        def _():
            gpart[t] = g

        @pl.when(q > 0)
        def _():
            gpart[t] += g

    def late_setup():
        f_copies[1].wait()
        f_copies[2].wait()
        block_two = f2[:, pl.ds(pl.multiple_of(col * 128, 128), 128)]
        u2n[...] = block_two.astype(BF16)
        u2w[...] = swapped(block_two, col)
        spread = (lax.broadcasted_iota(jnp.int32, (16, 128), 1) // 8 == lax.broadcasted_iota(jnp.int32, (16, 128), 0)).astype(BF16)
        r = lax.broadcasted_iota(jnp.int32, (width, 128), 0)
        l = lax.broadcasted_iota(jnp.int32, (width, 128), 1)

        def diagonal(which, q):
            u1 = f1[:, pl.ds(pl.multiple_of(which * 128, 128), 128)].astype(BF16)
            pick = (l == q * rows + r // 8).astype(BF16)
            rowed = lax.dot_general(pick, u1, NT, preferred_element_type=F32).astype(BF16)
            wide = jnp.dot(rowed, spread, preferred_element_type=F32)
            return jnp.where(r % 8 == l % 8, wide, 0.0).astype(BF16)

        for q in range(nq):
            w1[q] = diagonal(row, q)
        w1o[...] = diagonal(1 - row, nq - 1)

    def as_row(column, count):
        i = lax.broadcasted_iota(jnp.int32, (count, 128), 0)
        return jnp.sum(jnp.where(i == lax.broadcasted_iota(jnp.int32, (count, 128), 1), column, 0.0), axis=0, keepdims=True)

    def row_sums(blocks):
        return as_row(jnp.sum(jnp.sum(blocks, axis=1), axis=1, keepdims=True), blocks.shape[0])

    def step(s, carry):
        @pl.when((s > LAG) & (s <= nc))
        def _():
            y_copy(s - 1 - LAG).wait_send()

        @pl.when((s >= 2) & (s < nc))
        def _():
            y_copy(s - 1).start()

        @pl.when(s == nc)
        def _():
            for k in range(LAST):
                y_last(k).start()

        @pl.when(s < nc)
        def _():
            mode_three(s)

        @pl.when(s == 2)
        def _():
            late_setup()

        @pl.when(s == nc)
        def _():
            energy[0, :1] = row_sums(ex[...])

        @pl.when(s >= LAG)
        def _():
            mode_two(s - LAG)

        @pl.when(s >= LAG + 1)
        def _():
            mode_one(s - LAG - 1)

        return carry

    first = jnp.zeros((4, 8, 128), F32)
    for k in range(pieces):
        x_first[k].wait()
        if k == 0:
            f_copies[1].start()
            f_copies[2].start()
        elif k < XBUF:
            x_copy(k).start()
        first += block(0, 0, k)
        if k == 0:
            pl.semaphore_wait(barrier, 3)
        y_first(k).start()
    ex[0] = jnp.sum(first, axis=0)
    x_copy(XBUF).start()
    lax.fori_loop(1, nc + LAG - 1, step, 0)

    g_copy.start()
    far_first = (6, 7, 4, 5, 2, 3, 1)
    for k in range(LAST):
        if k == LAST - 1:
            mode_one(nc - 2)
            for dd in far_first:
                last_copy(dd).start()
        y_last(k).wait_recv()
        part = pl.ds(k * (rows // LAST), rows // LAST)
        a = (own[(nc - 1) % HELD, part] + yrecv[(nc - 1) % RING, part]).reshape(width // LAST, 128).astype(BF16)
        blast[0, k] = lax.dot_general(u2n[...], a, NT, preferred_element_type=F32)
        for dd in far_first:
            wide_copy(dd, k).start()
        if k == 0:
            g_copy.wait()
            g = gpart[early] + grecv[early]
            grecv[early] = g
            energy[0, 1:] = row_sums(g * g)
            for dd in range(1, 8):
                energy_copy(dd).start()
    for c in range(nc - LAG, nc - 1):
        y_copy(c).wait_send()
    tail = ysend.at[(nc - 1) % HELD]
    pltpu.make_async_copy(tail, tail, yls_sem.at[0]).wait()
    for c in range(nc - 1 - BHELD, nc - 1):
        b_copy(c).wait_send()
    wait_all(energy, 1, 8, all_send.at[2])
    wait_all(glast, 1, 8, all_send.at[1])

    def chip_pair(base):
        def summed(first):
            return jnp.concatenate([blast[first, k] + blast[first + 2, k] for k in range(LAST)], axis=1).astype(BF16)

        b_here, b_twin = summed(base), summed(base + 1)
        part = jnp.dot(b_here, w1[nq - 1], preferred_element_type=F32) + jnp.dot(b_twin, w1o[...], preferred_element_type=F32)
        low, high = part[:8], part[8:]
        return jnp.where(col == 0, low, high), jnp.where(col == 0, high, low)

    wait_all(glast, 1, 4, all_recv.at[2])
    wait_all(blast, 1, 4, all_recv.at[0])
    near = chip_pair(0)
    mine = (gpart[last] + glast[1]) + near[0]
    grecv[last] = mine
    for b in range(8):
        turned = grecv[:, b, :].T
        g_out[:, b] = jnp.where(row == 0, turned[:64], turned[64:]).reshape(8, 8, snaps)
    wait_all(energy, 1, 8, all_recv.at[4])
    x_energy = tree([energy[dd, :1] for dd in range(8)])
    g_energy = tree([energy[dd, 1:] for dd in (0, 2, 4, 6)])
    wait_all(blast, 1, 8, all_send.at[0])
    wait_all(glast, 4, 8, all_recv.at[3])
    wait_all(blast, 4, 8, all_recv.at[1])
    far = chip_pair(4)
    chips = [mine] + [(glast[dd] + glast[dd + 1]) + add for dd, add in ((2, near[1]), (4, far[0]), (6, far[1]))]
    final = jnp.sum(tree([g * g for g in chips]))
    g_energy = jnp.where(lax.broadcasted_iota(jnp.int32, (1, 128), 1) == last, final, g_energy)
    e_out[...] = ((x_energy - g_energy) / x_energy)[:, :snaps]


def finish(g_in, e_in, g_out, e_out, sem):
    copies = [pltpu.make_async_copy(g_in, g_out, sem.at[0]), pltpu.make_async_copy(e_in, e_out, sem.at[1])]
    for copy in copies:
        copy.start()
    for copy in copies:
        copy.wait()


def solution(mesh):
    rows = 64

    def local_part(x_block, f_one, f_two, f_three):
        snaps = x_block.shape[0]
        nq = 128 // rows
        nc = snaps * nq
        dma = pltpu.SemaphoreType.DMA
        hbm = pl.BlockSpec(memory_space=pltpu.HBM)
        vmem = pl.BlockSpec(memory_space=pltpu.VMEM)
        g, e = pl.pallas_call(
            functools.partial(kernel, snaps, rows),
            out_shape=(pltpu.VMEM((8, 8, 8, snaps), F32), pltpu.VMEM((1, snaps), F32)),
            in_specs=[hbm] * 4,
            out_specs=(vmem, vmem),
            scratch_shapes=[
                pltpu.VMEM((XBUF, rows * 128, 128), BF16),
                pltpu.VMEM((16, 256), F32), pltpu.VMEM((16, 256), F32), pltpu.VMEM((16, 256), F32),
                pltpu.VMEM((16, 128), BF16), pltpu.VMEM((16, 128), BF16),
                pltpu.VMEM((nq, rows * 8, 128), BF16),
                pltpu.VMEM((HELD, rows, 8, 128), F32), pltpu.VMEM((HELD, rows, 8, 128), F32), pltpu.VMEM((RING, rows, 8, 128), F32),
                pltpu.VMEM((BHELD, 8, rows * 8), F32), pltpu.VMEM((BHELD, 8, rows * 8), F32), pltpu.VMEM((BRING, 8, rows * 8), F32),
                pltpu.VMEM((snaps, 8, 128), F32), pltpu.VMEM((snaps, 8, 128), F32),
                pltpu.VMEM((snaps, 8, 128), F32), pltpu.VMEM((8, 2, 128), F32), pltpu.VMEM((8, 8, 128), F32),
                pltpu.VMEM((16, 128), BF16), pltpu.VMEM((rows * 8, 128), BF16), pltpu.VMEM((8, LAST, 16, rows * 8 // LAST), F32),
                dma((max(XBUF, rows // SUB),)), dma((LAG,)), dma((RING,)), dma((BHELD,)), dma((BRING,)), dma((1,)), dma((3,)), dma((5,)), dma((1,)), dma((LAST,)),
            ],
            compiler_params=pltpu.CompilerParams(collective_id=0, has_side_effects=True, vmem_limit_bytes=40 * 1024 * 1024),
        )(x_block.reshape(nc, rows * 128, 128), *(pltpu.with_memory_space_constraint(f.T, pltpu.HBM) for f in (f_one, f_two, f_three)))
        g, e = pl.pallas_call(
            finish,
            out_shape=(jax.ShapeDtypeStruct((8, 8, 8, snaps), F32), jax.ShapeDtypeStruct((1, snaps), F32)),
            in_specs=[vmem] * 2,
            out_specs=(hbm, hbm),
            scratch_shapes=[dma((2,))],
            compiler_params=pltpu.CompilerParams(vmem_limit_bytes=4 * 1024 * 1024),
        )(*(pltpu.with_memory_space_constraint(r, pltpu.VMEM) for r in (g, e)))
        return g.transpose(3, 0, 1, 2), e.reshape(snaps)

    return jax.shard_map(local_part, mesh=mesh, in_specs=(P(None, 'row', 'col', 'slab'), P(None, None), P(None, None), P(None, None)), out_specs=(P(None, 'row', 'col', 'slab'), P()), check_vma=False)
```

```python
import functools

import jax
import jax.numpy as jnp
from jax import lax
from jax.experimental import pallas as pl
from jax.experimental.pallas import tpu as pltpu
from jax.sharding import PartitionSpec as P

MESH = pl.DeviceIdType.MESH
F32, BF16 = jnp.float32, jnp.bfloat16
NT = (((1,), (1,)), ((), ()))

LAG = 3
RING = 2 * LAG
HELD = LAG + 1
XBUF = 4
BRING = 4
BHELD = 2
SUB = 8
LAST = 2


def other(axis):
    return {axis: 1 - lax.axis_index(axis)}


def offset_peer(dd):
    peer = {}
    for bit, axis in ((4, 'slab'), (2, 'col'), (1, 'row')):
        here = lax.axis_index(axis)
        peer[axis] = 1 - here if dd & bit else here
    return peer


def tree(parts):
    while len(parts) > 1:
        parts = [parts[k] + parts[k + 1] for k in range(0, len(parts), 2)]
    return parts[0]


def kernel(snaps, rows, x_hbm, f1_hbm, f2_hbm, f3_hbm, g_out, e_out,
           xbuf, f1, f2, f3, u3w, u2w, w1, own, ysend, yrecv, bown, xsend, xrecv,
           gpart, grecv, ex, energy, glast, u2n, w1o, blast, x_sem, ys_sem, yr_sem, xs_sem, xr_sem, g_sem, all_send, all_recv, yls_sem, ylr_sem):
    nq = 128 // rows
    nc = snaps * nq
    width = rows * 8
    last = snaps - 1
    slab, col, row = (lax.axis_index(a) for a in ('slab', 'col', 'row'))

    def x_copy(c):
        slot = lax.rem(c, XBUF)
        return pltpu.make_async_copy(x_hbm.at[c], xbuf.at[slot], x_sem.at[slot])

    f_copies = [pltpu.make_async_copy(src, dst, all_send.at[k]) for k, (src, dst) in enumerate(((f3_hbm, f3), (f2_hbm, f2), (f1_hbm, f1)))]
    pieces = rows // SUB
    x_first = [pltpu.make_async_copy(x_hbm.at[0, pl.ds(k * SUB * 128, SUB * 128)], xbuf.at[0, pl.ds(k * SUB * 128, SUB * 128)], x_sem.at[k]) for k in range(pieces)]
    x_first[0].start()
    f_copies[0].start()
    for copy in x_first[1:]:
        copy.start()

    barrier = pltpu.get_barrier_semaphore()
    for dd in (4, 2, 1):
        pl.semaphore_signal(barrier, inc=1, device_id=offset_peer(dd), device_id_type=MESH)

    def swapped(block, flip):
        return jnp.where(flip == 0, block, jnp.concatenate([block[8:], block[:8]], axis=0)).astype(BF16)

    f_copies[0].wait()
    u3w[...] = swapped(f3[:, pl.ds(pl.multiple_of(slab * 128, 128), 128)], slab)
    ex[...] = jnp.zeros_like(ex)

    def y_copy(c):
        held, slot = lax.rem(c, HELD), lax.rem(c, RING)
        return pltpu.make_async_remote_copy(ysend.at[held], yrecv.at[slot], ys_sem.at[lax.rem(c, LAG)], yr_sem.at[slot], device_id=other('slab'), device_id_type=MESH)

    def b_copy(c):
        held, slot = lax.rem(c, BHELD), lax.rem(c, BRING)
        return pltpu.make_async_remote_copy(xsend.at[held], xrecv.at[slot], xs_sem.at[held], xr_sem.at[slot], device_id=other('col'), device_id_type=MESH)

    def y_first(k):
        part = pl.ds(k * SUB, SUB)
        return pltpu.make_async_remote_copy(ysend.at[0, part], yrecv.at[0, part], ys_sem.at[0], yr_sem.at[0], device_id=other('slab'), device_id_type=MESH)

    def y_last(k):
        part = pl.ds(k * (rows // LAST), rows // LAST)
        return pltpu.make_async_remote_copy(ysend.at[(nc - 1) % HELD, part], yrecv.at[(nc - 1) % RING, part], yls_sem.at[0], ylr_sem.at[k], device_id=other('slab'), device_id_type=MESH)

    def wide_copy(dd, k):
        return pltpu.make_async_remote_copy(blast.at[0, k], blast.at[dd, k], all_send.at[0], all_recv.at[dd // 4], device_id=offset_peer(dd), device_id_type=MESH)

    def energy_copy(dd):
        return pltpu.make_async_remote_copy(energy.at[0], energy.at[dd], all_send.at[2], all_recv.at[4], device_id=offset_peer(dd), device_id_type=MESH)

    def last_copy(dd):
        return pltpu.make_async_remote_copy(gpart.at[last], glast.at[dd], all_send.at[1], all_recv.at[2 + dd // 4], device_id=offset_peer(dd), device_id_type=MESH)

    def wait_all(buffer, begin, end, sem):
        part = buffer.at[pl.ds(begin, end - begin)]
        pltpu.make_async_copy(part, part, sem).wait()

    early = pl.ds(0, last)
    g_copy = pltpu.make_async_remote_copy(gpart.at[early], grecv.at[early], all_send.at[2], g_sem.at[0], device_id=other('row'), device_id_type=MESH)

    def block(slot, xs, k):
        x = xbuf[xs, pl.ds(pl.multiple_of(k * SUB * 128, SUB * 128), SUB * 128), :]
        part = lax.dot_general(u3w[...], x, NT, preferred_element_type=F32)
        for i in range(SUB):
            own[slot, k * SUB + i] = part[:8, i * 128:(i + 1) * 128]
            ysend[slot, k * SUB + i] = part[8:, i * 128:(i + 1) * 128]
        xf = x.astype(F32).reshape(-1, 4, 8, 128)
        return jnp.sum(xf * xf, axis=0)

    def mode_three(c):
        slot, xs = lax.rem(c, HELD), lax.rem(c, XBUF)
        x_copy(c).wait()
        acc = lax.fori_loop(0, pieces, lambda k, acc: acc + block(slot, xs, k), jnp.zeros((4, 8, 128), F32))
        t = lax.div(c, nq)
        ex[t] += jnp.sum(acc, axis=0)

        @pl.when(c + XBUF < nc)
        def _():
            x_copy(c + XBUF).start()

    def mode_two(c):
        bslot = lax.rem(c, BHELD)

        @pl.when(c >= BHELD)
        def _():
            b_copy(c).wait_send()

        y_copy(c).wait_recv()
        a = (own[lax.rem(c, HELD)] + yrecv[lax.rem(c, RING)]).reshape(width, 128).astype(BF16)
        part = lax.dot_general(u2w[...], a, NT, preferred_element_type=F32)
        bown[bslot] = part[:8]
        xsend[bslot] = part[8:]
        b_copy(c).start()

    def mode_one(c):
        b_copy(c).wait_recv()
        b = (bown[lax.rem(c, BHELD)] + xrecv[lax.rem(c, BRING)]).astype(BF16)
        q, t = lax.rem(c, nq), lax.div(c, nq)
        g = jnp.dot(b, w1[q], preferred_element_type=F32)

        @pl.when(q == 0)
        def _():
            gpart[t] = g

        @pl.when(q > 0)
        def _():
            gpart[t] += g

    def late_setup():
        f_copies[1].wait()
        f_copies[2].wait()
        block_two = f2[:, pl.ds(pl.multiple_of(col * 128, 128), 128)]
        u2n[...] = block_two.astype(BF16)
        u2w[...] = swapped(block_two, col)
        spread = (lax.broadcasted_iota(jnp.int32, (16, 128), 1) // 8 == lax.broadcasted_iota(jnp.int32, (16, 128), 0)).astype(BF16)
        r = lax.broadcasted_iota(jnp.int32, (width, 128), 0)
        l = lax.broadcasted_iota(jnp.int32, (width, 128), 1)

        def diagonal(which, q):
            u1 = f1[:, pl.ds(pl.multiple_of(which * 128, 128), 128)].astype(BF16)
            pick = (l == q * rows + r // 8).astype(BF16)
            rowed = lax.dot_general(pick, u1, NT, preferred_element_type=F32).astype(BF16)
            wide = jnp.dot(rowed, spread, preferred_element_type=F32)
            return jnp.where(r % 8 == l % 8, wide, 0.0).astype(BF16)

        for q in range(nq):
            w1[q] = diagonal(row, q)
        w1o[...] = diagonal(1 - row, nq - 1)

    def as_row(column, count):
        i = lax.broadcasted_iota(jnp.int32, (count, 128), 0)
        return jnp.sum(jnp.where(i == lax.broadcasted_iota(jnp.int32, (count, 128), 1), column, 0.0), axis=0, keepdims=True)

    def row_sums(blocks):
        return as_row(jnp.sum(jnp.sum(blocks, axis=1), axis=1, keepdims=True), blocks.shape[0])

    def step(s, carry):
        @pl.when((s > LAG) & (s <= nc))
        def _():
            y_copy(s - 1 - LAG).wait_send()

        @pl.when((s >= 2) & (s < nc))
        def _():
            y_copy(s - 1).start()

        @pl.when(s == nc)
        def _():
            for c in range(nc - LAG, nc - 2):
                y_copy(c).wait_send()
            y_last(0).start()

        @pl.when(s == nc + 1)
        def _():
            y_copy(nc - 2).wait_send()
            y_last(1).start()

        @pl.when(s < nc)
        def _():
            mode_three(s)

        @pl.when(s == 2)
        def _():
            late_setup()

        @pl.when(s == nc)
        def _():
            energy[0, :1] = row_sums(ex[...])

        @pl.when(s == nc + LAG - 3)
        def _():
            g_copy.start()

        @pl.when(s >= LAG)
        def _():
            mode_two(s - LAG)

        @pl.when(s == nc + LAG - 2)
        def _():
            g_copy.wait()
            g = gpart[early] + grecv[early]
            grecv[early] = g
            energy[0, 1:] = row_sums(g * g)

        @pl.when(s >= LAG + 1)
        def _():
            mode_one(s - LAG - 1)

        return carry

    first = jnp.zeros((4, 8, 128), F32)
    for k in range(pieces):
        x_first[k].wait()
        if k == 0:
            f_copies[1].start()
            f_copies[2].start()
        else:
            x_copy(k).start()
        first += block(0, 0, k)
        if k == 0:
            pl.semaphore_wait(barrier, 3)
        y_first(k).start()
    ex[0] = jnp.sum(first, axis=0)
    x_copy(XBUF).start()
    lax.fori_loop(1, nc + LAG - 1, step, 0)

    for dd in range(1, 8):
        energy_copy(dd).start()
    far_first = (6, 7, 4, 5, 2, 3, 1)
    for k in range(LAST):
        if k == LAST - 1:
            mode_one(nc - 2)
            for dd in far_first:
                last_copy(dd).start()
        y_last(k).wait_recv()
        part = pl.ds(k * (rows // LAST), rows // LAST)
        a = (own[(nc - 1) % HELD, part] + yrecv[(nc - 1) % RING, part]).reshape(width // LAST, 128).astype(BF16)
        blast[0, k] = lax.dot_general(u2n[...], a, NT, preferred_element_type=F32)
        for dd in far_first:
            wide_copy(dd, k).start()
    tail = ysend.at[(nc - 1) % HELD]
    pltpu.make_async_copy(tail, tail, yls_sem.at[0]).wait()
    for c in range(nc - 1 - BHELD, nc - 1):
        b_copy(c).wait_send()
    wait_all(energy, 1, 8, all_send.at[2])
    wait_all(glast, 1, 8, all_send.at[1])

    def chip_pair(base):
        def summed(first):
            return jnp.concatenate([blast[first, k] + blast[first + 2, k] for k in range(LAST)], axis=1).astype(BF16)

        b_here, b_twin = summed(base), summed(base + 1)
        part = jnp.dot(b_here, w1[nq - 1], preferred_element_type=F32) + jnp.dot(b_twin, w1o[...], preferred_element_type=F32)
        low, high = part[:8], part[8:]
        return jnp.where(col == 0, low, high), jnp.where(col == 0, high, low)

    wait_all(glast, 1, 4, all_recv.at[2])
    wait_all(blast, 1, 4, all_recv.at[0])
    near = chip_pair(0)
    mine = (gpart[last] + glast[1]) + near[0]
    grecv[last] = mine
    for b in range(8):
        turned = grecv[:, b, :].T
        g_out[:, b] = jnp.where(row == 0, turned[:64], turned[64:]).reshape(8, 8, snaps)
    wait_all(energy, 1, 8, all_recv.at[4])
    x_energy = tree([energy[dd, :1] for dd in range(8)])
    g_energy = tree([energy[dd, 1:] for dd in (0, 2, 4, 6)])
    wait_all(blast, 1, 8, all_send.at[0])
    wait_all(glast, 4, 8, all_recv.at[3])
    wait_all(blast, 4, 8, all_recv.at[1])
    far = chip_pair(4)
    chips = [mine] + [(glast[dd] + glast[dd + 1]) + add for dd, add in ((2, near[1]), (4, far[0]), (6, far[1]))]
    final = jnp.sum(tree([g * g for g in chips]))
    g_energy = jnp.where(lax.broadcasted_iota(jnp.int32, (1, 128), 1) == last, final, g_energy)
    e_out[...] = ((x_energy - g_energy) / x_energy)[:, :snaps]


def finish(g_in, e_in, g_out, e_out, sem):
    copies = [pltpu.make_async_copy(g_in, g_out, sem.at[0]), pltpu.make_async_copy(e_in, e_out, sem.at[1])]
    for copy in copies:
        copy.start()
    for copy in copies:
        copy.wait()


def solution(mesh):
    rows = 32

    def local_part(x_block, f_one, f_two, f_three):
        snaps = x_block.shape[0]
        nq = 128 // rows
        nc = snaps * nq
        dma = pltpu.SemaphoreType.DMA
        hbm = pl.BlockSpec(memory_space=pltpu.HBM)
        vmem = pl.BlockSpec(memory_space=pltpu.VMEM)
        g, e = pl.pallas_call(
            functools.partial(kernel, snaps, rows),
            out_shape=(pltpu.VMEM((8, 8, 8, snaps), F32), pltpu.VMEM((1, snaps), F32)),
            in_specs=[hbm] * 4,
            out_specs=(vmem, vmem),
            scratch_shapes=[
                pltpu.VMEM((XBUF, rows * 128, 128), BF16),
                pltpu.VMEM((16, 256), F32), pltpu.VMEM((16, 256), F32), pltpu.VMEM((16, 256), F32),
                pltpu.VMEM((16, 128), BF16), pltpu.VMEM((16, 128), BF16),
                pltpu.VMEM((nq, rows * 8, 128), BF16),
                pltpu.VMEM((HELD, rows, 8, 128), F32), pltpu.VMEM((HELD, rows, 8, 128), F32), pltpu.VMEM((RING, rows, 8, 128), F32),
                pltpu.VMEM((BHELD, 8, rows * 8), F32), pltpu.VMEM((BHELD, 8, rows * 8), F32), pltpu.VMEM((BRING, 8, rows * 8), F32),
                pltpu.VMEM((snaps, 8, 128), F32), pltpu.VMEM((snaps, 8, 128), F32),
                pltpu.VMEM((snaps, 8, 128), F32), pltpu.VMEM((8, 2, 128), F32), pltpu.VMEM((8, 8, 128), F32),
                pltpu.VMEM((16, 128), BF16), pltpu.VMEM((rows * 8, 128), BF16), pltpu.VMEM((8, LAST, 16, rows * 8 // LAST), F32),
                dma((XBUF,)), dma((LAG,)), dma((RING,)), dma((BHELD,)), dma((BRING,)), dma((1,)), dma((3,)), dma((5,)), dma((1,)), dma((LAST,)),
            ],
            compiler_params=pltpu.CompilerParams(collective_id=0, has_side_effects=True, vmem_limit_bytes=40 * 1024 * 1024),
        )(x_block.reshape(nc, rows * 128, 128), *(pltpu.with_memory_space_constraint(f.T, pltpu.HBM) for f in (f_one, f_two, f_three)))
        g, e = pl.pallas_call(
            finish,
            out_shape=(jax.ShapeDtypeStruct((8, 8, 8, snaps), F32), jax.ShapeDtypeStruct((1, snaps), F32)),
            in_specs=[vmem] * 2,
            out_specs=(hbm, hbm),
            scratch_shapes=[dma((2,))],
            compiler_params=pltpu.CompilerParams(vmem_limit_bytes=4 * 1024 * 1024),
        )(*(pltpu.with_memory_space_constraint(r, pltpu.VMEM) for r in (g, e)))
        return g.transpose(3, 0, 1, 2), e.reshape(snaps)

    return jax.shard_map(local_part, mesh=mesh, in_specs=(P(None, 'row', 'col', 'slab'), P(None, None), P(None, None), P(None, None)), out_specs=(P(None, 'row', 'col', 'slab'), P()), check_vma=False)
```

```python
import functools

import jax
import jax.numpy as jnp
from jax import lax
from jax.experimental import pallas as pl
from jax.experimental.pallas import tpu as pltpu
from jax.sharding import PartitionSpec as P

MESH = pl.DeviceIdType.MESH
F32, BF16 = jnp.float32, jnp.bfloat16
NT = (((1,), (1,)), ((), ()))

LAG = 5
RING = 2 * LAG
HELD = LAG + 1
XBUF = 4
BRING = 4
BHELD = 2
SUB = 8
LAST = 2


def other(axis):
    return {axis: 1 - lax.axis_index(axis)}


def offset_peer(dd):
    peer = {}
    for bit, axis in ((4, 'slab'), (2, 'col'), (1, 'row')):
        here = lax.axis_index(axis)
        peer[axis] = 1 - here if dd & bit else here
    return peer


def tree(parts):
    while len(parts) > 1:
        parts = [parts[k] + parts[k + 1] for k in range(0, len(parts), 2)]
    return parts[0]


def kernel(snaps, rows, x_hbm, f1_hbm, f2_hbm, f3_hbm, g_out, e_out,
           xbuf, f1, f2, f3, u3w, u2w, w1, own, ysend, yrecv, bown, xsend, xrecv,
           gpart, grecv, ex, energy, glast, u2n, w1o, blast, x_sem, ys_sem, yr_sem, xs_sem, xr_sem, g_sem, all_send, all_recv, yls_sem, ylr_sem):
    nq = 128 // rows
    nc = snaps * nq
    width = rows * 8
    last = snaps - 1
    slab, col, row = (lax.axis_index(a) for a in ('slab', 'col', 'row'))

    def x_copy(c):
        slot = lax.rem(c, XBUF)
        return pltpu.make_async_copy(x_hbm.at[c], xbuf.at[slot], x_sem.at[slot])

    f_copies = [pltpu.make_async_copy(src, dst, all_send.at[k]) for k, (src, dst) in enumerate(((f3_hbm, f3), (f2_hbm, f2), (f1_hbm, f1)))]
    pieces = rows // SUB
    x_first = [pltpu.make_async_copy(x_hbm.at[0, pl.ds(k * SUB * 128, SUB * 128)], xbuf.at[0, pl.ds(k * SUB * 128, SUB * 128)], x_sem.at[k]) for k in range(pieces)]
    x_first[0].start()
    f_copies[0].start()
    for copy in x_first[1:]:
        copy.start()

    barrier = pltpu.get_barrier_semaphore()
    for dd in (4, 2, 1):
        pl.semaphore_signal(barrier, inc=1, device_id=offset_peer(dd), device_id_type=MESH)

    def swapped(block, flip):
        return jnp.where(flip == 0, block, jnp.concatenate([block[8:], block[:8]], axis=0)).astype(BF16)

    f_copies[0].wait()
    u3w[...] = swapped(f3[:, pl.ds(pl.multiple_of(slab * 128, 128), 128)], slab)
    ex[...] = jnp.zeros_like(ex)

    def y_copy(c):
        held, slot = lax.rem(c, HELD), lax.rem(c, RING)
        return pltpu.make_async_remote_copy(ysend.at[held], yrecv.at[slot], ys_sem.at[lax.rem(c, LAG)], yr_sem.at[slot], device_id=other('slab'), device_id_type=MESH)

    def b_copy(c):
        held, slot = lax.rem(c, BHELD), lax.rem(c, BRING)
        return pltpu.make_async_remote_copy(xsend.at[held], xrecv.at[slot], xs_sem.at[held], xr_sem.at[slot], device_id=other('col'), device_id_type=MESH)

    def y_first(k):
        part = pl.ds(k * SUB, SUB)
        return pltpu.make_async_remote_copy(ysend.at[0, part], yrecv.at[0, part], ys_sem.at[0], yr_sem.at[0], device_id=other('slab'), device_id_type=MESH)

    def y_last(k):
        part = pl.ds(k * (rows // LAST), rows // LAST)
        return pltpu.make_async_remote_copy(ysend.at[(nc - 1) % HELD, part], yrecv.at[(nc - 1) % RING, part], yls_sem.at[0], ylr_sem.at[k], device_id=other('slab'), device_id_type=MESH)

    def wide_copy(dd, k):
        return pltpu.make_async_remote_copy(blast.at[0, k], blast.at[dd, k], all_send.at[0], all_recv.at[dd // 4], device_id=offset_peer(dd), device_id_type=MESH)

    def energy_copy(dd):
        return pltpu.make_async_remote_copy(energy.at[0], energy.at[dd], all_send.at[2], all_recv.at[4], device_id=offset_peer(dd), device_id_type=MESH)

    def last_copy(dd):
        return pltpu.make_async_remote_copy(gpart.at[last], glast.at[dd], all_send.at[1], all_recv.at[2 + dd // 4], device_id=offset_peer(dd), device_id_type=MESH)

    def wait_all(buffer, begin, end, sem):
        part = buffer.at[pl.ds(begin, end - begin)]
        pltpu.make_async_copy(part, part, sem).wait()

    early = pl.ds(0, last)
    g_copy = pltpu.make_async_remote_copy(gpart.at[early], grecv.at[early], all_send.at[2], g_sem.at[0], device_id=other('row'), device_id_type=MESH)

    def block(slot, xs, k):
        x = xbuf[xs, pl.ds(pl.multiple_of(k * SUB * 128, SUB * 128), SUB * 128), :]
        part = lax.dot_general(u3w[...], x, NT, preferred_element_type=F32)
        for i in range(SUB):
            own[slot, k * SUB + i] = part[:8, i * 128:(i + 1) * 128]
            ysend[slot, k * SUB + i] = part[8:, i * 128:(i + 1) * 128]
        xf = x.astype(F32).reshape(-1, 4, 8, 128)
        return jnp.sum(xf * xf, axis=0)

    def mode_three(c):
        slot, xs = lax.rem(c, HELD), lax.rem(c, XBUF)
        x_copy(c).wait()
        acc = lax.fori_loop(0, pieces, lambda k, acc: acc + block(slot, xs, k), jnp.zeros((4, 8, 128), F32))
        t = lax.div(c, nq)
        ex[t] += jnp.sum(acc, axis=0)

        @pl.when(c + XBUF < nc)
        def _():
            x_copy(c + XBUF).start()

    def mode_two(c):
        bslot = lax.rem(c, BHELD)

        @pl.when(c >= BHELD)
        def _():
            b_copy(c).wait_send()

        y_copy(c).wait_recv()
        a = (own[lax.rem(c, HELD)] + yrecv[lax.rem(c, RING)]).reshape(width, 128).astype(BF16)
        part = lax.dot_general(u2w[...], a, NT, preferred_element_type=F32)
        bown[bslot] = part[:8]
        xsend[bslot] = part[8:]
        b_copy(c).start()

    def mode_one(c):
        b_copy(c).wait_recv()
        b = (bown[lax.rem(c, BHELD)] + xrecv[lax.rem(c, BRING)]).astype(BF16)
        q, t = lax.rem(c, nq), lax.div(c, nq)
        g = jnp.dot(b, w1[q], preferred_element_type=F32)

        @pl.when(q == 0)
        def _():
            gpart[t] = g

        @pl.when(q > 0)
        def _():
            gpart[t] += g

    def late_setup():
        f_copies[1].wait()
        f_copies[2].wait()
        block_two = f2[:, pl.ds(pl.multiple_of(col * 128, 128), 128)]
        u2n[...] = block_two.astype(BF16)
        u2w[...] = swapped(block_two, col)
        spread = (lax.broadcasted_iota(jnp.int32, (16, 128), 1) // 8 == lax.broadcasted_iota(jnp.int32, (16, 128), 0)).astype(BF16)
        r = lax.broadcasted_iota(jnp.int32, (width, 128), 0)
        l = lax.broadcasted_iota(jnp.int32, (width, 128), 1)

        def diagonal(which, q):
            u1 = f1[:, pl.ds(pl.multiple_of(which * 128, 128), 128)].astype(BF16)
            pick = (l == q * rows + r // 8).astype(BF16)
            rowed = lax.dot_general(pick, u1, NT, preferred_element_type=F32).astype(BF16)
            wide = jnp.dot(rowed, spread, preferred_element_type=F32)
            return jnp.where(r % 8 == l % 8, wide, 0.0).astype(BF16)

        for q in range(nq):
            w1[q] = diagonal(row, q)
        w1o[...] = diagonal(1 - row, nq - 1)

    def as_row(column, count):
        i = lax.broadcasted_iota(jnp.int32, (count, 128), 0)
        return jnp.sum(jnp.where(i == lax.broadcasted_iota(jnp.int32, (count, 128), 1), column, 0.0), axis=0, keepdims=True)

    def row_sums(blocks):
        return as_row(jnp.sum(jnp.sum(blocks, axis=1), axis=1, keepdims=True), blocks.shape[0])

    def step(s, carry):
        @pl.when((s > LAG) & (s <= nc))
        def _():
            y_copy(s - 1 - LAG).wait_send()

        @pl.when((s >= 2) & (s < nc))
        def _():
            y_copy(s - 1).start()

        @pl.when(s == nc)
        def _():
            for k in range(LAST):
                y_last(k).start()

        @pl.when(s < nc)
        def _():
            mode_three(s)

        @pl.when(s == 2)
        def _():
            late_setup()

        @pl.when(s == nc)
        def _():
            energy[0, :1] = row_sums(ex[...])

        @pl.when(s == nc + LAG - 3)
        def _():
            g_copy.start()

        @pl.when(s >= LAG)
        def _():
            mode_two(s - LAG)

        @pl.when(s == nc + LAG - 2)
        def _():
            g_copy.wait()
            g = gpart[early] + grecv[early]
            grecv[early] = g
            energy[0, 1:] = row_sums(g * g)

        @pl.when(s >= LAG + 1)
        def _():
            mode_one(s - LAG - 1)

        return carry

    first = jnp.zeros((4, 8, 128), F32)
    for k in range(pieces):
        x_first[k].wait()
        if k == 0:
            f_copies[1].start()
            f_copies[2].start()
        else:
            x_copy(k).start()
        first += block(0, 0, k)
        if k == 0:
            pl.semaphore_wait(barrier, 3)
        y_first(k).start()
    ex[0] = jnp.sum(first, axis=0)
    x_copy(XBUF).start()
    lax.fori_loop(1, nc + LAG - 1, step, 0)

    for dd in range(1, 8):
        energy_copy(dd).start()
    far_first = (6, 7, 4, 5, 2, 3, 1)
    for k in range(LAST):
        if k == LAST - 1:
            mode_one(nc - 2)
            for dd in far_first:
                last_copy(dd).start()
        y_last(k).wait_recv()
        part = pl.ds(k * (rows // LAST), rows // LAST)
        a = (own[(nc - 1) % HELD, part] + yrecv[(nc - 1) % RING, part]).reshape(width // LAST, 128).astype(BF16)
        blast[0, k] = lax.dot_general(u2n[...], a, NT, preferred_element_type=F32)
        for dd in far_first:
            wide_copy(dd, k).start()
    for c in range(nc - LAG, nc - 1):
        y_copy(c).wait_send()
    tail = ysend.at[(nc - 1) % HELD]
    pltpu.make_async_copy(tail, tail, yls_sem.at[0]).wait()
    for c in range(nc - 1 - BHELD, nc - 1):
        b_copy(c).wait_send()
    wait_all(energy, 1, 8, all_send.at[2])
    wait_all(glast, 1, 8, all_send.at[1])

    def chip_pair(base):
        def summed(first):
            return jnp.concatenate([blast[first, k] + blast[first + 2, k] for k in range(LAST)], axis=1).astype(BF16)

        b_here, b_twin = summed(base), summed(base + 1)
        part = jnp.dot(b_here, w1[nq - 1], preferred_element_type=F32) + jnp.dot(b_twin, w1o[...], preferred_element_type=F32)
        low, high = part[:8], part[8:]
        return jnp.where(col == 0, low, high), jnp.where(col == 0, high, low)

    wait_all(glast, 1, 4, all_recv.at[2])
    wait_all(blast, 1, 4, all_recv.at[0])
    near = chip_pair(0)
    mine = (gpart[last] + glast[1]) + near[0]
    grecv[last] = mine
    for b in range(8):
        turned = grecv[:, b, :].T
        g_out[:, b] = jnp.where(row == 0, turned[:64], turned[64:]).reshape(8, 8, snaps)
    wait_all(energy, 1, 8, all_recv.at[4])
    x_energy = tree([energy[dd, :1] for dd in range(8)])
    g_energy = tree([energy[dd, 1:] for dd in (0, 2, 4, 6)])
    wait_all(blast, 1, 8, all_send.at[0])
    wait_all(glast, 4, 8, all_recv.at[3])
    wait_all(blast, 4, 8, all_recv.at[1])
    far = chip_pair(4)
    chips = [mine] + [(glast[dd] + glast[dd + 1]) + add for dd, add in ((2, near[1]), (4, far[0]), (6, far[1]))]
    final = jnp.sum(tree([g * g for g in chips]))
    g_energy = jnp.where(lax.broadcasted_iota(jnp.int32, (1, 128), 1) == last, final, g_energy)
    e_out[...] = ((x_energy - g_energy) / x_energy)[:, :snaps]


def finish(g_in, e_in, g_out, e_out, sem):
    copies = [pltpu.make_async_copy(g_in, g_out, sem.at[0]), pltpu.make_async_copy(e_in, e_out, sem.at[1])]
    for copy in copies:
        copy.start()
    for copy in copies:
        copy.wait()


def solution(mesh):
    rows = 32

    def local_part(x_block, f_one, f_two, f_three):
        snaps = x_block.shape[0]
        nq = 128 // rows
        nc = snaps * nq
        dma = pltpu.SemaphoreType.DMA
        hbm = pl.BlockSpec(memory_space=pltpu.HBM)
        vmem = pl.BlockSpec(memory_space=pltpu.VMEM)
        g, e = pl.pallas_call(
            functools.partial(kernel, snaps, rows),
            out_shape=(pltpu.VMEM((8, 8, 8, snaps), F32), pltpu.VMEM((1, snaps), F32)),
            in_specs=[hbm] * 4,
            out_specs=(vmem, vmem),
            scratch_shapes=[
                pltpu.VMEM((XBUF, rows * 128, 128), BF16),
                pltpu.VMEM((16, 256), F32), pltpu.VMEM((16, 256), F32), pltpu.VMEM((16, 256), F32),
                pltpu.VMEM((16, 128), BF16), pltpu.VMEM((16, 128), BF16),
                pltpu.VMEM((nq, rows * 8, 128), BF16),
                pltpu.VMEM((HELD, rows, 8, 128), F32), pltpu.VMEM((HELD, rows, 8, 128), F32), pltpu.VMEM((RING, rows, 8, 128), F32),
                pltpu.VMEM((BHELD, 8, rows * 8), F32), pltpu.VMEM((BHELD, 8, rows * 8), F32), pltpu.VMEM((BRING, 8, rows * 8), F32),
                pltpu.VMEM((snaps, 8, 128), F32), pltpu.VMEM((snaps, 8, 128), F32),
                pltpu.VMEM((snaps, 8, 128), F32), pltpu.VMEM((8, 2, 128), F32), pltpu.VMEM((8, 8, 128), F32),
                pltpu.VMEM((16, 128), BF16), pltpu.VMEM((rows * 8, 128), BF16), pltpu.VMEM((8, LAST, 16, rows * 8 // LAST), F32),
                dma((XBUF,)), dma((LAG,)), dma((RING,)), dma((BHELD,)), dma((BRING,)), dma((1,)), dma((3,)), dma((5,)), dma((1,)), dma((LAST,)),
            ],
            compiler_params=pltpu.CompilerParams(collective_id=0, has_side_effects=True, vmem_limit_bytes=40 * 1024 * 1024),
        )(x_block.reshape(nc, rows * 128, 128), *(pltpu.with_memory_space_constraint(f.T, pltpu.HBM) for f in (f_one, f_two, f_three)))
        g, e = pl.pallas_call(
            finish,
            out_shape=(jax.ShapeDtypeStruct((8, 8, 8, snaps), F32), jax.ShapeDtypeStruct((1, snaps), F32)),
            in_specs=[vmem] * 2,
            out_specs=(hbm, hbm),
            scratch_shapes=[dma((2,))],
            compiler_params=pltpu.CompilerParams(vmem_limit_bytes=4 * 1024 * 1024),
        )(*(pltpu.with_memory_space_constraint(r, pltpu.VMEM) for r in (g, e)))
        return g.transpose(3, 0, 1, 2), e.reshape(snaps)

    return jax.shard_map(local_part, mesh=mesh, in_specs=(P(None, 'row', 'col', 'slab'), P(None, None), P(None, None), P(None, None)), out_specs=(P(None, 'row', 'col', 'slab'), P()), check_vma=False)
```

```python
import functools

import jax
import jax.numpy as jnp
from jax import lax
from jax.experimental import pallas as pl
from jax.experimental.pallas import tpu as pltpu
from jax.sharding import PartitionSpec as P

MESH = pl.DeviceIdType.MESH
F32, BF16 = jnp.float32, jnp.bfloat16
NT = (((1,), (1,)), ((), ()))

LAG = 3
RING = 2 * LAG
HELD = LAG + 1
XBUF = 4
BRING = 4
BHELD = 2
SUB = 8
LAST = 2


def other(axis):
    return {axis: 1 - lax.axis_index(axis)}


def offset_peer(dd):
    peer = {}
    for bit, axis in ((4, 'slab'), (2, 'col'), (1, 'row')):
        here = lax.axis_index(axis)
        peer[axis] = 1 - here if dd & bit else here
    return peer


def tree(parts):
    while len(parts) > 1:
        parts = [parts[k] + parts[k + 1] for k in range(0, len(parts), 2)]
    return parts[0]


def kernel(snaps, rows, x_hbm, f1_hbm, f2_hbm, f3_hbm, g_out, e_out,
           xbuf, f1, f2, f3, u3w, u2w, w1, own, ysend, yrecv, bown, xsend, xrecv,
           gpart, grecv, ex, energy, glast, u2n, w1o, blast, x_sem, ys_sem, yr_sem, xs_sem, xr_sem, g_sem, all_send, all_recv, ylr_sem):
    nq = 128 // rows
    nc = snaps * nq
    width = rows * 8
    last = snaps - 1
    slab, col, row = (lax.axis_index(a) for a in ('slab', 'col', 'row'))

    def x_copy(c):
        slot = lax.rem(c, XBUF)
        return pltpu.make_async_copy(x_hbm.at[c], xbuf.at[slot], x_sem.at[slot])

    f_copies = [pltpu.make_async_copy(src, dst, all_send.at[k]) for k, (src, dst) in enumerate(((f3_hbm, f3), (f2_hbm, f2), (f1_hbm, f1)))]
    pieces = rows // SUB
    x_first = [pltpu.make_async_copy(x_hbm.at[0, pl.ds(k * SUB * 128, SUB * 128)], xbuf.at[0, pl.ds(k * SUB * 128, SUB * 128)], x_sem.at[k]) for k in range(pieces)]
    x_first[0].start()
    f_copies[0].start()
    for copy in x_first[1:]:
        copy.start()

    barrier = pltpu.get_barrier_semaphore()
    for dd in (4, 2, 1):
        pl.semaphore_signal(barrier, inc=1, device_id=offset_peer(dd), device_id_type=MESH)

    def swapped(block, flip):
        return jnp.where(flip == 0, block, jnp.concatenate([block[8:], block[:8]], axis=0)).astype(BF16)

    f_copies[0].wait()
    u3w[...] = swapped(f3[:, pl.ds(pl.multiple_of(slab * 128, 128), 128)], slab)
    ex[...] = jnp.zeros_like(ex)

    def y_copy(c):
        held, slot = lax.rem(c, HELD), lax.rem(c, RING)
        return pltpu.make_async_remote_copy(ysend.at[held], yrecv.at[slot], ys_sem.at[lax.rem(c, LAG)], yr_sem.at[slot], device_id=other('slab'), device_id_type=MESH)

    def b_copy(c):
        held, slot = lax.rem(c, BHELD), lax.rem(c, BRING)
        return pltpu.make_async_remote_copy(xsend.at[held], xrecv.at[slot], xs_sem.at[held], xr_sem.at[slot], device_id=other('col'), device_id_type=MESH)

    def y_first(k):
        part = pl.ds(k * SUB, SUB)
        return pltpu.make_async_remote_copy(ysend.at[0, part], yrecv.at[0, part], ys_sem.at[0], yr_sem.at[0], device_id=other('slab'), device_id_type=MESH)

    def y_last(k):
        part = pl.ds(k * (rows // LAST), rows // LAST)
        return pltpu.make_async_remote_copy(ysend.at[(nc - 1) % HELD, part], yrecv.at[(nc - 1) % RING, part], ys_sem.at[(nc - 1) % LAG], yr_sem.at[(nc - 1) % RING] if k == 0 else ylr_sem.at[k - 1], device_id=other('slab'), device_id_type=MESH)

    def wide_copy(dd, k):
        return pltpu.make_async_remote_copy(blast.at[0, k], blast.at[dd, k], all_send.at[0], all_recv.at[dd // 4], device_id=offset_peer(dd), device_id_type=MESH)

    def energy_copy(dd):
        return pltpu.make_async_remote_copy(energy.at[0], energy.at[dd], all_send.at[2], all_recv.at[4], device_id=offset_peer(dd), device_id_type=MESH)

    def last_copy(dd):
        return pltpu.make_async_remote_copy(gpart.at[last], glast.at[dd], all_send.at[1], all_recv.at[2 + dd // 4], device_id=offset_peer(dd), device_id_type=MESH)

    def wait_all(buffer, begin, end, sem):
        part = buffer.at[pl.ds(begin, end - begin)]
        pltpu.make_async_copy(part, part, sem).wait()

    early = pl.ds(0, last)
    g_copy = pltpu.make_async_remote_copy(gpart.at[early], grecv.at[early], all_send.at[2], g_sem.at[0], device_id=other('row'), device_id_type=MESH)

    def block(slot, xs, k):
        x = xbuf[xs, pl.ds(pl.multiple_of(k * SUB * 128, SUB * 128), SUB * 128), :]
        part = lax.dot_general(u3w[...], x, NT, preferred_element_type=F32)
        for i in range(SUB):
            own[slot, k * SUB + i] = part[:8, i * 128:(i + 1) * 128]
            ysend[slot, k * SUB + i] = part[8:, i * 128:(i + 1) * 128]
        xf = x.astype(F32).reshape(-1, 4, 8, 128)
        return jnp.sum(xf * xf, axis=0)

    def mode_three(c):
        slot, xs = lax.rem(c, HELD), lax.rem(c, XBUF)
        x_copy(c).wait()
        acc = lax.fori_loop(0, pieces, lambda k, acc: acc + block(slot, xs, k), jnp.zeros((4, 8, 128), F32))
        t = lax.div(c, nq)
        ex[t] += jnp.sum(acc, axis=0)

        @pl.when(c + XBUF < nc)
        def _():
            x_copy(c + XBUF).start()

    def mode_two(c):
        bslot = lax.rem(c, BHELD)

        @pl.when(c >= BHELD)
        def _():
            b_copy(c).wait_send()

        y_copy(c).wait_recv()
        a = (own[lax.rem(c, HELD)] + yrecv[lax.rem(c, RING)]).reshape(width, 128).astype(BF16)
        part = lax.dot_general(u2w[...], a, NT, preferred_element_type=F32)
        bown[bslot] = part[:8]
        xsend[bslot] = part[8:]
        b_copy(c).start()

    def mode_one(c):
        b_copy(c).wait_recv()
        b = (bown[lax.rem(c, BHELD)] + xrecv[lax.rem(c, BRING)]).astype(BF16)
        q, t = lax.rem(c, nq), lax.div(c, nq)
        g = jnp.dot(b, w1[q], preferred_element_type=F32)

        @pl.when(q == 0)
        def _():
            gpart[t] = g

        @pl.when(q > 0)
        def _():
            gpart[t] += g

    def late_setup():
        f_copies[1].wait()
        f_copies[2].wait()
        block_two = f2[:, pl.ds(pl.multiple_of(col * 128, 128), 128)]
        u2n[...] = block_two.astype(BF16)
        u2w[...] = swapped(block_two, col)
        spread = (lax.broadcasted_iota(jnp.int32, (16, 128), 1) // 8 == lax.broadcasted_iota(jnp.int32, (16, 128), 0)).astype(BF16)
        r = lax.broadcasted_iota(jnp.int32, (width, 128), 0)
        l = lax.broadcasted_iota(jnp.int32, (width, 128), 1)

        def diagonal(which, q):
            u1 = f1[:, pl.ds(pl.multiple_of(which * 128, 128), 128)].astype(BF16)
            pick = (l == q * rows + r // 8).astype(BF16)
            rowed = lax.dot_general(pick, u1, NT, preferred_element_type=F32).astype(BF16)
            wide = jnp.dot(rowed, spread, preferred_element_type=F32)
            return jnp.where(r % 8 == l % 8, wide, 0.0).astype(BF16)

        for q in range(nq):
            w1[q] = diagonal(row, q)
        w1o[...] = diagonal(1 - row, nq - 1)

    def as_row(column, count):
        i = lax.broadcasted_iota(jnp.int32, (count, 128), 0)
        return jnp.sum(jnp.where(i == lax.broadcasted_iota(jnp.int32, (count, 128), 1), column, 0.0), axis=0, keepdims=True)

    def row_sums(blocks):
        return as_row(jnp.sum(jnp.sum(blocks, axis=1), axis=1, keepdims=True), blocks.shape[0])

    def step(s, carry):
        @pl.when((s > LAG) & (s <= nc))
        def _():
            y_copy(s - 1 - LAG).wait_send()

        @pl.when((s >= 2) & (s < nc))
        def _():
            y_copy(s - 1).start()

        @pl.when(s == nc)
        def _():
            for k in range(LAST):
                y_last(k).start()

        @pl.when(s < nc)
        def _():
            mode_three(s)

        @pl.when(s == 2)
        def _():
            late_setup()

        @pl.when(s == nc)
        def _():
            energy[0, :1] = row_sums(ex[...])

        @pl.when(s == nc + LAG - 3)
        def _():
            g_copy.start()

        @pl.when(s >= LAG)
        def _():
            mode_two(s - LAG)

        @pl.when(s == nc + LAG - 2)
        def _():
            g_copy.wait()
            g = gpart[early] + grecv[early]
            grecv[early] = g
            energy[0, 1:] = row_sums(g * g)

        @pl.when(s >= LAG + 1)
        def _():
            mode_one(s - LAG - 1)

        return carry

    first = jnp.zeros((4, 8, 128), F32)
    for k in range(pieces):
        x_first[k].wait()
        if k == 0:
            f_copies[1].start()
            f_copies[2].start()
        else:
            x_copy(k).start()
        first += block(0, 0, k)
        if k == 0:
            pl.semaphore_wait(barrier, 3)
        y_first(k).start()
    ex[0] = jnp.sum(first, axis=0)
    x_copy(XBUF).start()
    lax.fori_loop(1, nc + LAG - 1, step, 0)

    for dd in range(1, 8):
        energy_copy(dd).start()
    far_first = (6, 7, 4, 5, 2, 3, 1)
    for k in range(LAST):
        if k == LAST - 1:
            mode_one(nc - 2)
            for dd in far_first:
                last_copy(dd).start()
        y_last(k).wait_recv()
        part = pl.ds(k * (rows // LAST), rows // LAST)
        a = (own[(nc - 1) % HELD, part] + yrecv[(nc - 1) % RING, part]).reshape(width // LAST, 128).astype(BF16)
        blast[0, k] = lax.dot_general(u2n[...], a, NT, preferred_element_type=F32)
        for dd in far_first:
            wide_copy(dd, k).start()

    def chip_pair(base):
        def summed(first):
            return jnp.concatenate([blast[first, k] + blast[first + 2, k] for k in range(LAST)], axis=1).astype(BF16)

        b_here, b_twin = summed(base), summed(base + 1)
        part = jnp.dot(b_here, w1[nq - 1], preferred_element_type=F32) + jnp.dot(b_twin, w1o[...], preferred_element_type=F32)
        low, high = part[:8], part[8:]
        return jnp.where(col == 0, low, high), jnp.where(col == 0, high, low)

    wait_all(glast, 1, 4, all_recv.at[2])
    wait_all(blast, 1, 4, all_recv.at[0])
    near = chip_pair(0)
    mine = (gpart[last] + glast[1]) + near[0]
    grecv[last] = mine
    for b in range(8):
        turned = grecv[:, b, :].T
        g_out[:, b] = jnp.where(row == 0, turned[:64], turned[64:]).reshape(8, 8, snaps)
    wait_all(energy, 1, 8, all_recv.at[4])
    x_energy = tree([energy[dd, :1] for dd in range(8)])
    g_energy = tree([energy[dd, 1:] for dd in (0, 2, 4, 6)])
    wait_all(glast, 4, 8, all_recv.at[3])
    wait_all(blast, 4, 8, all_recv.at[1])
    far = chip_pair(4)
    chips = [mine] + [(glast[dd] + glast[dd + 1]) + add for dd, add in ((2, near[1]), (4, far[0]), (6, far[1]))]
    final = jnp.sum(jnp.sum(tree([g * g for g in chips]), axis=0, keepdims=True), axis=1, keepdims=True)
    g_energy = jnp.where(lax.broadcasted_iota(jnp.int32, (1, 128), 1) == last, final, g_energy)
    e_out[...] = ((x_energy - g_energy) / x_energy)[:, :snaps]

    for c in range(nc - LAG, nc):
        y_copy(c).wait_send()
    for c in range(nc - 1 - BHELD, nc - 1):
        b_copy(c).wait_send()
    wait_all(energy, 1, 8, all_send.at[2])
    wait_all(glast, 1, 8, all_send.at[1])
    wait_all(blast, 1, 8, all_send.at[0])


def finish(g_in, e_in, g_out, e_out, sem):
    copies = [pltpu.make_async_copy(g_in, g_out, sem.at[0]), pltpu.make_async_copy(e_in, e_out, sem.at[1])]
    for copy in copies:
        copy.start()
    for copy in copies:
        copy.wait()


def solution(mesh):
    rows = 32

    def local_part(x_block, f_one, f_two, f_three):
        snaps = x_block.shape[0]
        nq = 128 // rows
        nc = snaps * nq
        dma = pltpu.SemaphoreType.DMA
        hbm = pl.BlockSpec(memory_space=pltpu.HBM)
        vmem = pl.BlockSpec(memory_space=pltpu.VMEM)
        g, e = pl.pallas_call(
            functools.partial(kernel, snaps, rows),
            out_shape=(pltpu.VMEM((8, 8, 8, snaps), F32), pltpu.VMEM((1, snaps), F32)),
            in_specs=[hbm] * 4,
            out_specs=(vmem, vmem),
            scratch_shapes=[
                pltpu.VMEM((XBUF, rows * 128, 128), BF16),
                pltpu.VMEM((16, 256), F32), pltpu.VMEM((16, 256), F32), pltpu.VMEM((16, 256), F32),
                pltpu.VMEM((16, 128), BF16), pltpu.VMEM((16, 128), BF16),
                pltpu.VMEM((nq, rows * 8, 128), BF16),
                pltpu.VMEM((HELD, rows, 8, 128), F32), pltpu.VMEM((HELD, rows, 8, 128), F32), pltpu.VMEM((RING, rows, 8, 128), F32),
                pltpu.VMEM((BHELD, 8, rows * 8), F32), pltpu.VMEM((BHELD, 8, rows * 8), F32), pltpu.VMEM((BRING, 8, rows * 8), F32),
                pltpu.VMEM((snaps, 8, 128), F32), pltpu.VMEM((snaps, 8, 128), F32),
                pltpu.VMEM((snaps, 8, 128), F32), pltpu.VMEM((8, 2, 128), F32), pltpu.VMEM((8, 8, 128), F32),
                pltpu.VMEM((16, 128), BF16), pltpu.VMEM((rows * 8, 128), BF16), pltpu.VMEM((8, LAST, 16, rows * 8 // LAST), F32),
                dma((XBUF,)), dma((LAG,)), dma((RING,)), dma((BHELD,)), dma((BRING,)), dma((1,)), dma((3,)), dma((5,)), dma((LAST - 1,)),
            ],
            compiler_params=pltpu.CompilerParams(collective_id=0, has_side_effects=True, vmem_limit_bytes=40 * 1024 * 1024),
        )(x_block.reshape(nc, rows * 128, 128), *(pltpu.with_memory_space_constraint(f.T, pltpu.HBM) for f in (f_one, f_two, f_three)))
        g, e = pl.pallas_call(
            finish,
            out_shape=(jax.ShapeDtypeStruct((8, 8, 8, snaps), F32), jax.ShapeDtypeStruct((1, snaps), F32)),
            in_specs=[vmem] * 2,
            out_specs=(hbm, hbm),
            scratch_shapes=[dma((2,))],
            compiler_params=pltpu.CompilerParams(vmem_limit_bytes=4 * 1024 * 1024),
        )(*(pltpu.with_memory_space_constraint(r, pltpu.VMEM) for r in (g, e)))
        return g.transpose(3, 0, 1, 2), e.reshape(snaps)

    return jax.shard_map(local_part, mesh=mesh, in_specs=(P(None, 'row', 'col', 'slab'), P(None, None), P(None, None), P(None, None)), out_specs=(P(None, 'row', 'col', 'slab'), P()), check_vma=False)
```

```python
import functools

import jax
import jax.numpy as jnp
from jax import lax
from jax.experimental import pallas as pl
from jax.experimental.pallas import tpu as pltpu
from jax.sharding import PartitionSpec as P

MESH = pl.DeviceIdType.MESH
F32, BF16 = jnp.float32, jnp.bfloat16
NT = (((1,), (1,)), ((), ()))

LAG = 3
RING = 2 * LAG
HELD = LAG + 1
XBUF = 4
BRING = 4
BHELD = 2
SUB = 8
LAST = 2


def other(axis):
    return {axis: 1 - lax.axis_index(axis)}


def offset_peer(dd):
    peer = {}
    for bit, axis in ((4, 'slab'), (2, 'col'), (1, 'row')):
        here = lax.axis_index(axis)
        peer[axis] = 1 - here if dd & bit else here
    return peer


def tree(parts):
    while len(parts) > 1:
        parts = [parts[k] + parts[k + 1] for k in range(0, len(parts), 2)]
    return parts[0]


def kernel(snaps, rows, x_hbm, f1_hbm, f2_hbm, f3_hbm, g_out, e_out,
           xbuf, f1, f2, f3, u3w, u2w, w1, own, ysend, yrecv, bown, xsend, xrecv,
           gpart, grecv, ex, energy, glast, u2n, w1o, blast, x_sem, ys_sem, yr_sem, xs_sem, xr_sem, g_sem, all_send, all_recv, ylr_sem):
    nq = 128 // rows
    nc = snaps * nq
    width = rows * 8
    last = snaps - 1
    slab, col, row = (lax.axis_index(a) for a in ('slab', 'col', 'row'))

    def x_copy(c):
        slot = lax.rem(c, XBUF)
        return pltpu.make_async_copy(x_hbm.at[c], xbuf.at[slot], x_sem.at[slot])

    f_copies = [pltpu.make_async_copy(src, dst, all_send.at[k]) for k, (src, dst) in enumerate(((f3_hbm, f3), (f2_hbm, f2), (f1_hbm, f1)))]
    pieces = rows // SUB
    x_first = [pltpu.make_async_copy(x_hbm.at[0, pl.ds(k * SUB * 128, SUB * 128)], xbuf.at[0, pl.ds(k * SUB * 128, SUB * 128)], x_sem.at[k]) for k in range(pieces)]
    x_first[0].start()
    f_copies[0].start()
    for copy in x_first[1:]:
        copy.start()

    barrier = pltpu.get_barrier_semaphore()
    for dd in (4, 2, 1):
        pl.semaphore_signal(barrier, inc=1, device_id=offset_peer(dd), device_id_type=MESH)

    def swapped(block, flip):
        return jnp.where(flip == 0, block, jnp.concatenate([block[8:], block[:8]], axis=0)).astype(BF16)

    f_copies[0].wait()
    u3w[...] = swapped(f3[:, pl.ds(pl.multiple_of(slab * 128, 128), 128)], slab)
    ex[...] = jnp.zeros_like(ex)

    def y_copy(c):
        held, slot = lax.rem(c, HELD), lax.rem(c, RING)
        return pltpu.make_async_remote_copy(ysend.at[held], yrecv.at[slot], ys_sem.at[lax.rem(c, LAG)], yr_sem.at[slot], device_id=other('slab'), device_id_type=MESH)

    def b_copy(c):
        held, slot = lax.rem(c, BHELD), lax.rem(c, BRING)
        return pltpu.make_async_remote_copy(xsend.at[held], xrecv.at[slot], xs_sem.at[held], xr_sem.at[slot], device_id=other('col'), device_id_type=MESH)

    def y_first(k):
        part = pl.ds(k * SUB, SUB)
        return pltpu.make_async_remote_copy(ysend.at[0, part], yrecv.at[0, part], ys_sem.at[0], yr_sem.at[0], device_id=other('slab'), device_id_type=MESH)

    def y_last(k):
        part = pl.ds(k * (rows // LAST), rows // LAST)
        return pltpu.make_async_remote_copy(ysend.at[(nc - 1) % HELD, part], yrecv.at[(nc - 1) % RING, part], ys_sem.at[(nc - 1) % LAG], yr_sem.at[(nc - 1) % RING] if k == 0 else ylr_sem.at[k - 1], device_id=other('slab'), device_id_type=MESH)

    def to_each(send):
        for dest in range(8):
            place = {'slab': dest // 4, 'col': dest // 2 % 2, 'row': dest % 2}
            bits = [lax.axis_index(a) if there == 0 else 1 - lax.axis_index(a) for a, there in place.items()]
            slot = bits[0] * 4 + bits[1] * 2 + bits[2]

            @pl.when(slot > 0)
            def _():
                send(slot, bits[0], place).start()

    def wide_copy(k):
        return lambda slot, far, place: pltpu.make_async_remote_copy(blast.at[0, k], blast.at[slot, k], all_send.at[0], all_recv.at[far], device_id=place, device_id_type=MESH)

    def energy_copy(slot, far, place):
        return pltpu.make_async_remote_copy(energy.at[0], energy.at[slot], all_send.at[2], all_recv.at[4], device_id=place, device_id_type=MESH)

    def last_copy(slot, far, place):
        return pltpu.make_async_remote_copy(gpart.at[last], glast.at[slot], all_send.at[1], all_recv.at[2 + far], device_id=place, device_id_type=MESH)

    def wait_all(buffer, begin, end, sem):
        part = buffer.at[pl.ds(begin, end - begin)]
        pltpu.make_async_copy(part, part, sem).wait()

    early = pl.ds(0, last)
    g_copy = pltpu.make_async_remote_copy(gpart.at[early], grecv.at[early], all_send.at[2], g_sem.at[0], device_id=other('row'), device_id_type=MESH)

    def block(slot, xs, k):
        x = xbuf[xs, pl.ds(pl.multiple_of(k * SUB * 128, SUB * 128), SUB * 128), :]
        part = lax.dot_general(u3w[...], x, NT, preferred_element_type=F32)
        for i in range(SUB):
            own[slot, k * SUB + i] = part[:8, i * 128:(i + 1) * 128]
            ysend[slot, k * SUB + i] = part[8:, i * 128:(i + 1) * 128]
        xf = x.astype(F32).reshape(-1, 4, 8, 128)
        return jnp.sum(xf * xf, axis=0)

    def mode_three(c):
        slot, xs = lax.rem(c, HELD), lax.rem(c, XBUF)
        x_copy(c).wait()
        acc = lax.fori_loop(0, pieces, lambda k, acc: acc + block(slot, xs, k), jnp.zeros((4, 8, 128), F32))
        t = lax.div(c, nq)
        ex[t] += jnp.sum(acc, axis=0)

        @pl.when(c + XBUF < nc)
        def _():
            x_copy(c + XBUF).start()

    def mode_two(c):
        bslot = lax.rem(c, BHELD)

        @pl.when(c >= BHELD)
        def _():
            b_copy(c).wait_send()

        y_copy(c).wait_recv()
        a = (own[lax.rem(c, HELD)] + yrecv[lax.rem(c, RING)]).reshape(width, 128).astype(BF16)
        part = lax.dot_general(u2w[...], a, NT, preferred_element_type=F32)
        bown[bslot] = part[:8]
        xsend[bslot] = part[8:]
        b_copy(c).start()

    def mode_one(c):
        b_copy(c).wait_recv()
        b = (bown[lax.rem(c, BHELD)] + xrecv[lax.rem(c, BRING)]).astype(BF16)
        q, t = lax.rem(c, nq), lax.div(c, nq)
        g = jnp.dot(b, w1[q], preferred_element_type=F32)

        @pl.when(q == 0)
        def _():
            gpart[t] = g

        @pl.when(q > 0)
        def _():
            gpart[t] += g

    def late_setup():
        f_copies[1].wait()
        f_copies[2].wait()
        block_two = f2[:, pl.ds(pl.multiple_of(col * 128, 128), 128)]
        u2n[...] = block_two.astype(BF16)
        u2w[...] = swapped(block_two, col)
        spread = (lax.broadcasted_iota(jnp.int32, (16, 128), 1) // 8 == lax.broadcasted_iota(jnp.int32, (16, 128), 0)).astype(BF16)
        r = lax.broadcasted_iota(jnp.int32, (width, 128), 0)
        l = lax.broadcasted_iota(jnp.int32, (width, 128), 1)

        def diagonal(which, q):
            u1 = f1[:, pl.ds(pl.multiple_of(which * 128, 128), 128)].astype(BF16)
            pick = (l == q * rows + r // 8).astype(BF16)
            rowed = lax.dot_general(pick, u1, NT, preferred_element_type=F32).astype(BF16)
            wide = jnp.dot(rowed, spread, preferred_element_type=F32)
            return jnp.where(r % 8 == l % 8, wide, 0.0).astype(BF16)

        for q in range(nq):
            w1[q] = diagonal(row, q)
        w1o[...] = diagonal(1 - row, nq - 1)

    def as_row(column, count):
        i = lax.broadcasted_iota(jnp.int32, (count, 128), 0)
        return jnp.sum(jnp.where(i == lax.broadcasted_iota(jnp.int32, (count, 128), 1), column, 0.0), axis=0, keepdims=True)

    def row_sums(blocks):
        return as_row(jnp.sum(jnp.sum(blocks, axis=1), axis=1, keepdims=True), blocks.shape[0])

    def step(s, carry):
        @pl.when((s > LAG) & (s <= nc))
        def _():
            y_copy(s - 1 - LAG).wait_send()

        @pl.when((s >= 2) & (s < nc))
        def _():
            y_copy(s - 1).start()

        @pl.when(s == nc)
        def _():
            for k in range(LAST):
                y_last(k).start()

        @pl.when(s < nc)
        def _():
            mode_three(s)

        @pl.when(s == 2)
        def _():
            late_setup()

        @pl.when(s == nc)
        def _():
            energy[0, :1] = row_sums(ex[...])

        @pl.when(s == nc + LAG - 3)
        def _():
            g_copy.start()

        @pl.when(s >= LAG)
        def _():
            mode_two(s - LAG)

        @pl.when(s == nc + LAG - 2)
        def _():
            g_copy.wait()
            g = gpart[early] + grecv[early]
            grecv[early] = g
            energy[0, 1:] = row_sums(g * g)

        @pl.when(s >= LAG + 1)
        def _():
            mode_one(s - LAG - 1)

        return carry

    first = jnp.zeros((4, 8, 128), F32)
    for k in range(pieces):
        x_first[k].wait()
        if k == 0:
            f_copies[1].start()
            f_copies[2].start()
        else:
            x_copy(k).start()
        first += block(0, 0, k)
        if k == 0:
            pl.semaphore_wait(barrier, 3)
        y_first(k).start()
    ex[0] = jnp.sum(first, axis=0)
    x_copy(XBUF).start()
    lax.fori_loop(1, nc + LAG - 1, step, 0)

    to_each(energy_copy)
    for k in range(LAST):
        if k == LAST - 1:
            mode_one(nc - 2)
            to_each(last_copy)
        y_last(k).wait_recv()
        part = pl.ds(k * (rows // LAST), rows // LAST)
        a = (own[(nc - 1) % HELD, part] + yrecv[(nc - 1) % RING, part]).reshape(width // LAST, 128).astype(BF16)
        blast[0, k] = lax.dot_general(u2n[...], a, NT, preferred_element_type=F32)
        to_each(wide_copy(k))

    def chip_pair(base):
        def summed(first):
            return jnp.concatenate([blast[first, k] + blast[first + 2, k] for k in range(LAST)], axis=1).astype(BF16)

        b_here, b_twin = summed(base), summed(base + 1)
        part = jnp.dot(b_here, w1[nq - 1], preferred_element_type=F32) + jnp.dot(b_twin, w1o[...], preferred_element_type=F32)
        low, high = part[:8], part[8:]
        return jnp.where(col == 0, low, high), jnp.where(col == 0, high, low)

    wait_all(glast, 1, 4, all_recv.at[2])
    wait_all(blast, 1, 4, all_recv.at[0])
    near = chip_pair(0)
    mine = (gpart[last] + glast[1]) + near[0]
    grecv[last] = mine
    for b in range(8):
        turned = grecv[:, b, :].T
        g_out[:, b] = jnp.where(row == 0, turned[:64], turned[64:]).reshape(8, 8, snaps)
    wait_all(energy, 1, 8, all_recv.at[4])
    x_energy = tree([energy[dd, :1] for dd in range(8)])
    g_energy = tree([energy[dd, 1:] for dd in (0, 2, 4, 6)])
    wait_all(glast, 4, 8, all_recv.at[3])
    wait_all(blast, 4, 8, all_recv.at[1])
    far = chip_pair(4)
    chips = [mine] + [(glast[dd] + glast[dd + 1]) + add for dd, add in ((2, near[1]), (4, far[0]), (6, far[1]))]
    final = jnp.sum(jnp.sum(tree([g * g for g in chips]), axis=0, keepdims=True), axis=1, keepdims=True)
    g_energy = jnp.where(lax.broadcasted_iota(jnp.int32, (1, 128), 1) == last, final, g_energy)
    e_out[...] = ((x_energy - g_energy) / x_energy)[:, :snaps]

    for c in range(nc - LAG, nc):
        y_copy(c).wait_send()
    for c in range(nc - 1 - BHELD, nc - 1):
        b_copy(c).wait_send()
    wait_all(energy, 1, 8, all_send.at[2])
    wait_all(glast, 1, 8, all_send.at[1])
    wait_all(blast, 1, 8, all_send.at[0])


def finish(g_in, e_in, g_out, e_out, sem):
    copies = [pltpu.make_async_copy(g_in, g_out, sem.at[0]), pltpu.make_async_copy(e_in, e_out, sem.at[1])]
    for copy in copies:
        copy.start()
    for copy in copies:
        copy.wait()


def solution(mesh):
    rows = 32

    def local_part(x_block, f_one, f_two, f_three):
        snaps = x_block.shape[0]
        nq = 128 // rows
        nc = snaps * nq
        dma = pltpu.SemaphoreType.DMA
        hbm = pl.BlockSpec(memory_space=pltpu.HBM)
        vmem = pl.BlockSpec(memory_space=pltpu.VMEM)
        g, e = pl.pallas_call(
            functools.partial(kernel, snaps, rows),
            out_shape=(pltpu.VMEM((8, 8, 8, snaps), F32), pltpu.VMEM((1, snaps), F32)),
            in_specs=[hbm] * 4,
            out_specs=(vmem, vmem),
            scratch_shapes=[
                pltpu.VMEM((XBUF, rows * 128, 128), BF16),
                pltpu.VMEM((16, 256), F32), pltpu.VMEM((16, 256), F32), pltpu.VMEM((16, 256), F32),
                pltpu.VMEM((16, 128), BF16), pltpu.VMEM((16, 128), BF16),
                pltpu.VMEM((nq, rows * 8, 128), BF16),
                pltpu.VMEM((HELD, rows, 8, 128), F32), pltpu.VMEM((HELD, rows, 8, 128), F32), pltpu.VMEM((RING, rows, 8, 128), F32),
                pltpu.VMEM((BHELD, 8, rows * 8), F32), pltpu.VMEM((BHELD, 8, rows * 8), F32), pltpu.VMEM((BRING, 8, rows * 8), F32),
                pltpu.VMEM((snaps, 8, 128), F32), pltpu.VMEM((snaps, 8, 128), F32),
                pltpu.VMEM((snaps, 8, 128), F32), pltpu.VMEM((8, 2, 128), F32), pltpu.VMEM((8, 8, 128), F32),
                pltpu.VMEM((16, 128), BF16), pltpu.VMEM((rows * 8, 128), BF16), pltpu.VMEM((8, LAST, 16, rows * 8 // LAST), F32),
                dma((XBUF,)), dma((LAG,)), dma((RING,)), dma((BHELD,)), dma((BRING,)), dma((1,)), dma((3,)), dma((5,)), dma((LAST - 1,)),
            ],
            compiler_params=pltpu.CompilerParams(collective_id=0, has_side_effects=True, vmem_limit_bytes=40 * 1024 * 1024),
        )(x_block.reshape(nc, rows * 128, 128), *(pltpu.with_memory_space_constraint(f.T, pltpu.HBM) for f in (f_one, f_two, f_three)))
        g, e = pl.pallas_call(
            finish,
            out_shape=(jax.ShapeDtypeStruct((8, 8, 8, snaps), F32), jax.ShapeDtypeStruct((1, snaps), F32)),
            in_specs=[vmem] * 2,
            out_specs=(hbm, hbm),
            scratch_shapes=[dma((2,))],
            compiler_params=pltpu.CompilerParams(vmem_limit_bytes=4 * 1024 * 1024),
        )(*(pltpu.with_memory_space_constraint(r, pltpu.VMEM) for r in (g, e)))
        return g.transpose(3, 0, 1, 2), e.reshape(snaps)

    return jax.shard_map(local_part, mesh=mesh, in_specs=(P(None, 'row', 'col', 'slab'), P(None, None), P(None, None), P(None, None)), out_specs=(P(None, 'row', 'col', 'slab'), P()), check_vma=False)
```

```python
import functools

import jax
import jax.numpy as jnp
from jax import lax
from jax.experimental import pallas as pl
from jax.experimental.pallas import tpu as pltpu
from jax.sharding import PartitionSpec as P

MESH = pl.DeviceIdType.MESH
F32, BF16 = jnp.float32, jnp.bfloat16
NT = (((1,), (1,)), ((), ()))

LAG = 3
RING = 2 * LAG
HELD = LAG + 1
XBUF = 4
BRING = 4
BHELD = 2
SUB = 8
LAST = 2
FIRST = (0, 2, 8, 16, 24, 32)


def other(axis):
    return {axis: 1 - lax.axis_index(axis)}


def offset_peer(dd):
    peer = {}
    for bit, axis in ((4, 'slab'), (2, 'col'), (1, 'row')):
        here = lax.axis_index(axis)
        peer[axis] = 1 - here if dd & bit else here
    return peer


def tree(parts):
    while len(parts) > 1:
        parts = [parts[k] + parts[k + 1] for k in range(0, len(parts), 2)]
    return parts[0]


def kernel(snaps, rows, x_hbm, f1_hbm, f2_hbm, f3_hbm, g_out, e_out,
           xbuf, f1, f2, f3, u3w, u2w, w1, own, ysend, yrecv, bown, xsend, xrecv,
           gpart, grecv, ex, energy, glast, u2n, w1o, blast, x_sem, ys_sem, yr_sem, xs_sem, xr_sem, g_sem, all_send, all_recv, ylr_sem):
    nq = 128 // rows
    nc = snaps * nq
    width = rows * 8
    last = snaps - 1
    slab, col, row = (lax.axis_index(a) for a in ('slab', 'col', 'row'))

    def x_copy(c):
        slot = lax.rem(c, XBUF)
        return pltpu.make_async_copy(x_hbm.at[c], xbuf.at[slot], x_sem.at[slot])

    f_copies = [pltpu.make_async_copy(src, dst, all_send.at[k]) for k, (src, dst) in enumerate(((f3_hbm, f3), (f2_hbm, f2), (f1_hbm, f1)))]
    pieces = rows // SUB
    spans = list(zip(FIRST[:-1], FIRST[1:]))
    x_first = []
    for k, (begin, end) in enumerate(spans):
        part = pl.ds(begin * 128, (end - begin) * 128)
        x_first.append(pltpu.make_async_copy(x_hbm.at[0, part], xbuf.at[0, part], x_sem.at[k] if k < XBUF else xs_sem.at[k - XBUF]))
    x_first[0].start()
    f_copies[0].start()
    for copy in x_first[1:]:
        copy.start()

    barrier = pltpu.get_barrier_semaphore()
    for dd in (4, 2, 1):
        pl.semaphore_signal(barrier, inc=1, device_id=offset_peer(dd), device_id_type=MESH)

    def swapped(block, flip):
        return jnp.where(flip == 0, block, jnp.concatenate([block[8:], block[:8]], axis=0)).astype(BF16)

    f_copies[0].wait()
    u3w[...] = swapped(f3[:, pl.ds(pl.multiple_of(slab * 128, 128), 128)], slab)
    ex[...] = jnp.zeros_like(ex)

    def y_copy(c):
        held, slot = lax.rem(c, HELD), lax.rem(c, RING)
        return pltpu.make_async_remote_copy(ysend.at[held], yrecv.at[slot], ys_sem.at[lax.rem(c, LAG)], yr_sem.at[slot], device_id=other('slab'), device_id_type=MESH)

    def b_copy(c):
        held, slot = lax.rem(c, BHELD), lax.rem(c, BRING)
        return pltpu.make_async_remote_copy(xsend.at[held], xrecv.at[slot], xs_sem.at[held], xr_sem.at[slot], device_id=other('col'), device_id_type=MESH)

    def y_first(k):
        begin, end = spans[k]
        part = pl.ds(begin, end - begin)
        return pltpu.make_async_remote_copy(ysend.at[0, part], yrecv.at[0, part], ys_sem.at[0], yr_sem.at[0], device_id=other('slab'), device_id_type=MESH)

    def y_last(k):
        part = pl.ds(k * (rows // LAST), rows // LAST)
        return pltpu.make_async_remote_copy(ysend.at[(nc - 1) % HELD, part], yrecv.at[(nc - 1) % RING, part], ys_sem.at[(nc - 1) % LAG], yr_sem.at[(nc - 1) % RING] if k == 0 else ylr_sem.at[k - 1], device_id=other('slab'), device_id_type=MESH)

    def to_each(send):
        for dest in range(8):
            place = {'slab': dest // 4, 'col': dest // 2 % 2, 'row': dest % 2}
            bits = [lax.axis_index(a) if there == 0 else 1 - lax.axis_index(a) for a, there in place.items()]
            slot = bits[0] * 4 + bits[1] * 2 + bits[2]

            @pl.when(slot > 0)
            def _():
                send(slot, bits[0], place).start()

    def wide_copy(k):
        return lambda slot, far, place: pltpu.make_async_remote_copy(blast.at[0, k], blast.at[slot, k], all_send.at[0], all_recv.at[far], device_id=place, device_id_type=MESH)

    def energy_copy(slot, far, place):
        return pltpu.make_async_remote_copy(energy.at[0], energy.at[slot], all_send.at[2], all_recv.at[4], device_id=place, device_id_type=MESH)

    def last_copy(slot, far, place):
        return pltpu.make_async_remote_copy(gpart.at[last], glast.at[slot], all_send.at[1], all_recv.at[2 + far], device_id=place, device_id_type=MESH)

    def wait_all(buffer, begin, end, sem):
        part = buffer.at[pl.ds(begin, end - begin)]
        pltpu.make_async_copy(part, part, sem).wait()

    early = pl.ds(0, last)
    g_copy = pltpu.make_async_remote_copy(gpart.at[early], grecv.at[early], all_send.at[2], g_sem.at[0], device_id=other('row'), device_id_type=MESH)

    def block(slot, xs, begin, count):
        x = xbuf[xs, pl.ds(begin * 128, count * 128), :]
        part = lax.dot_general(u3w[...], x, NT, preferred_element_type=F32)
        for i in range(count):
            own[slot, begin + i] = part[:8, i * 128:(i + 1) * 128]
            ysend[slot, begin + i] = part[8:, i * 128:(i + 1) * 128]
        xf = x.astype(F32).reshape(-1, 4, 8, 128)
        return jnp.sum(xf * xf, axis=0)

    def mode_three(c):
        slot, xs = lax.rem(c, HELD), lax.rem(c, XBUF)
        x_copy(c).wait()
        acc = lax.fori_loop(0, pieces, lambda k, acc: acc + block(slot, xs, pl.multiple_of(k * SUB, SUB), SUB), jnp.zeros((4, 8, 128), F32))
        t = lax.div(c, nq)
        ex[t] += jnp.sum(acc, axis=0)

        @pl.when(c + XBUF < nc)
        def _():
            x_copy(c + XBUF).start()

    def mode_two(c):
        bslot = lax.rem(c, BHELD)

        @pl.when(c >= BHELD)
        def _():
            b_copy(c).wait_send()

        y_copy(c).wait_recv()
        a = (own[lax.rem(c, HELD)] + yrecv[lax.rem(c, RING)]).reshape(width, 128).astype(BF16)
        part = lax.dot_general(u2w[...], a, NT, preferred_element_type=F32)
        bown[bslot] = part[:8]
        xsend[bslot] = part[8:]
        b_copy(c).start()

    def mode_one(c):
        b_copy(c).wait_recv()
        b = (bown[lax.rem(c, BHELD)] + xrecv[lax.rem(c, BRING)]).astype(BF16)
        q, t = lax.rem(c, nq), lax.div(c, nq)
        g = jnp.dot(b, w1[q], preferred_element_type=F32)

        @pl.when(q == 0)
        def _():
            gpart[t] = g

        @pl.when(q > 0)
        def _():
            gpart[t] += g

    def late_setup():
        f_copies[1].wait()
        f_copies[2].wait()
        block_two = f2[:, pl.ds(pl.multiple_of(col * 128, 128), 128)]
        u2n[...] = block_two.astype(BF16)
        u2w[...] = swapped(block_two, col)
        spread = (lax.broadcasted_iota(jnp.int32, (16, 128), 1) // 8 == lax.broadcasted_iota(jnp.int32, (16, 128), 0)).astype(BF16)
        r = lax.broadcasted_iota(jnp.int32, (width, 128), 0)
        l = lax.broadcasted_iota(jnp.int32, (width, 128), 1)

        def diagonal(which, q):
            u1 = f1[:, pl.ds(pl.multiple_of(which * 128, 128), 128)].astype(BF16)
            pick = (l == q * rows + r // 8).astype(BF16)
            rowed = lax.dot_general(pick, u1, NT, preferred_element_type=F32).astype(BF16)
            wide = jnp.dot(rowed, spread, preferred_element_type=F32)
            return jnp.where(r % 8 == l % 8, wide, 0.0).astype(BF16)

        for q in range(nq):
            w1[q] = diagonal(row, q)
        w1o[...] = diagonal(1 - row, nq - 1)

    def as_row(column, count):
        i = lax.broadcasted_iota(jnp.int32, (count, 128), 0)
        return jnp.sum(jnp.where(i == lax.broadcasted_iota(jnp.int32, (count, 128), 1), column, 0.0), axis=0, keepdims=True)

    def row_sums(blocks):
        return as_row(jnp.sum(jnp.sum(blocks, axis=1), axis=1, keepdims=True), blocks.shape[0])

    def step(s, carry):
        @pl.when((s > LAG) & (s <= nc))
        def _():
            y_copy(s - 1 - LAG).wait_send()

        @pl.when((s >= 2) & (s < nc))
        def _():
            y_copy(s - 1).start()

        @pl.when(s == nc)
        def _():
            for k in range(LAST):
                y_last(k).start()

        @pl.when(s < nc)
        def _():
            mode_three(s)

        @pl.when(s == 2)
        def _():
            late_setup()

        @pl.when(s == nc)
        def _():
            energy[0, :1] = row_sums(ex[...])

        @pl.when(s == nc + LAG - 3)
        def _():
            g_copy.start()

        @pl.when(s >= LAG)
        def _():
            mode_two(s - LAG)

        @pl.when(s == nc + LAG - 2)
        def _():
            g_copy.wait()
            g = gpart[early] + grecv[early]
            grecv[early] = g
            energy[0, 1:] = row_sums(g * g)

        @pl.when(s >= LAG + 1)
        def _():
            mode_one(s - LAG - 1)

        return carry

    first = jnp.zeros((4, 8, 128), F32)
    for k, (begin, end) in enumerate(spans):
        x_first[k].wait()
        if k == 0:
            f_copies[1].start()
            f_copies[2].start()
        elif k < XBUF:
            x_copy(k).start()
        first += block(0, 0, begin, end - begin)
        if k == 0:
            pl.semaphore_wait(barrier, 3)
        y_first(k).start()
    ex[0] = jnp.sum(first, axis=0)
    x_copy(XBUF).start()
    lax.fori_loop(1, nc + LAG - 1, step, 0)

    to_each(energy_copy)
    for k in range(LAST):
        if k == LAST - 1:
            mode_one(nc - 2)
            to_each(last_copy)
        y_last(k).wait_recv()
        part = pl.ds(k * (rows // LAST), rows // LAST)
        a = (own[(nc - 1) % HELD, part] + yrecv[(nc - 1) % RING, part]).reshape(width // LAST, 128).astype(BF16)
        blast[0, k] = lax.dot_general(u2n[...], a, NT, preferred_element_type=F32)
        to_each(wide_copy(k))

    def chip_pair(base):
        def summed(first):
            return jnp.concatenate([blast[first, k] + blast[first + 2, k] for k in range(LAST)], axis=1).astype(BF16)

        b_here, b_twin = summed(base), summed(base + 1)
        part = jnp.dot(b_here, w1[nq - 1], preferred_element_type=F32) + jnp.dot(b_twin, w1o[...], preferred_element_type=F32)
        low, high = part[:8], part[8:]
        return jnp.where(col == 0, low, high), jnp.where(col == 0, high, low)

    wait_all(glast, 1, 4, all_recv.at[2])
    wait_all(blast, 1, 4, all_recv.at[0])
    near = chip_pair(0)
    mine = (gpart[last] + glast[1]) + near[0]
    grecv[last] = mine
    for b in range(8):
        turned = grecv[:, b, :].T
        g_out[:, b] = jnp.where(row == 0, turned[:64], turned[64:]).reshape(8, 8, snaps)
    wait_all(energy, 1, 8, all_recv.at[4])
    x_energy = tree([energy[dd, :1] for dd in range(8)])
    g_energy = tree([energy[dd, 1:] for dd in (0, 2, 4, 6)])
    wait_all(glast, 4, 8, all_recv.at[3])
    wait_all(blast, 4, 8, all_recv.at[1])
    far = chip_pair(4)
    chips = [mine] + [(glast[dd] + glast[dd + 1]) + add for dd, add in ((2, near[1]), (4, far[0]), (6, far[1]))]
    final = jnp.sum(jnp.sum(tree([g * g for g in chips]), axis=0, keepdims=True), axis=1, keepdims=True)
    g_energy = jnp.where(lax.broadcasted_iota(jnp.int32, (1, 128), 1) == last, final, g_energy)
    e_out[...] = ((x_energy - g_energy) / x_energy)[:, :snaps]

    for c in range(nc - LAG, nc):
        y_copy(c).wait_send()
    for c in range(nc - 1 - BHELD, nc - 1):
        b_copy(c).wait_send()
    wait_all(energy, 1, 8, all_send.at[2])
    wait_all(glast, 1, 8, all_send.at[1])
    wait_all(blast, 1, 8, all_send.at[0])


def finish(g_in, e_in, g_out, e_out, sem):
    copies = [pltpu.make_async_copy(g_in, g_out, sem.at[0]), pltpu.make_async_copy(e_in, e_out, sem.at[1])]
    for copy in copies:
        copy.start()
    for copy in copies:
        copy.wait()


def solution(mesh):
    rows = 32

    def local_part(x_block, f_one, f_two, f_three):
        snaps = x_block.shape[0]
        nq = 128 // rows
        nc = snaps * nq
        dma = pltpu.SemaphoreType.DMA
        hbm = pl.BlockSpec(memory_space=pltpu.HBM)
        vmem = pl.BlockSpec(memory_space=pltpu.VMEM)
        g, e = pl.pallas_call(
            functools.partial(kernel, snaps, rows),
            out_shape=(pltpu.VMEM((8, 8, 8, snaps), F32), pltpu.VMEM((1, snaps), F32)),
            in_specs=[hbm] * 4,
            out_specs=(vmem, vmem),
            scratch_shapes=[
                pltpu.VMEM((XBUF, rows * 128, 128), BF16),
                pltpu.VMEM((16, 256), F32), pltpu.VMEM((16, 256), F32), pltpu.VMEM((16, 256), F32),
                pltpu.VMEM((16, 128), BF16), pltpu.VMEM((16, 128), BF16),
                pltpu.VMEM((nq, rows * 8, 128), BF16),
                pltpu.VMEM((HELD, rows, 8, 128), F32), pltpu.VMEM((HELD, rows, 8, 128), F32), pltpu.VMEM((RING, rows, 8, 128), F32),
                pltpu.VMEM((BHELD, 8, rows * 8), F32), pltpu.VMEM((BHELD, 8, rows * 8), F32), pltpu.VMEM((BRING, 8, rows * 8), F32),
                pltpu.VMEM((snaps, 8, 128), F32), pltpu.VMEM((snaps, 8, 128), F32),
                pltpu.VMEM((snaps, 8, 128), F32), pltpu.VMEM((8, 2, 128), F32), pltpu.VMEM((8, 8, 128), F32),
                pltpu.VMEM((16, 128), BF16), pltpu.VMEM((rows * 8, 128), BF16), pltpu.VMEM((8, LAST, 16, rows * 8 // LAST), F32),
                dma((XBUF,)), dma((LAG,)), dma((RING,)), dma((BHELD,)), dma((BRING,)), dma((1,)), dma((3,)), dma((5,)), dma((LAST - 1,)),
            ],
            compiler_params=pltpu.CompilerParams(collective_id=0, has_side_effects=True, vmem_limit_bytes=40 * 1024 * 1024),
        )(x_block.reshape(nc, rows * 128, 128), *(pltpu.with_memory_space_constraint(f.T, pltpu.HBM) for f in (f_one, f_two, f_three)))
        g, e = pl.pallas_call(
            finish,
            out_shape=(jax.ShapeDtypeStruct((8, 8, 8, snaps), F32), jax.ShapeDtypeStruct((1, snaps), F32)),
            in_specs=[vmem] * 2,
            out_specs=(hbm, hbm),
            scratch_shapes=[dma((2,))],
            compiler_params=pltpu.CompilerParams(vmem_limit_bytes=4 * 1024 * 1024),
        )(*(pltpu.with_memory_space_constraint(r, pltpu.VMEM) for r in (g, e)))
        return g.transpose(3, 0, 1, 2), e.reshape(snaps)

    return jax.shard_map(local_part, mesh=mesh, in_specs=(P(None, 'row', 'col', 'slab'), P(None, None), P(None, None), P(None, None)), out_specs=(P(None, 'row', 'col', 'slab'), P()), check_vma=False)
```

```python
import functools

import jax
import jax.numpy as jnp
from jax import lax
from jax.experimental import pallas as pl
from jax.experimental.pallas import tpu as pltpu
from jax.sharding import PartitionSpec as P

MESH = pl.DeviceIdType.MESH
F32, BF16 = jnp.float32, jnp.bfloat16
NT = (((1,), (1,)), ((), ()))

LAG = 3
RING = 2 * LAG
HELD = LAG + 1
XBUF = 2
BRING = 4
BHELD = 2
SUB = 8
LAST = 2
FIRST = (0, 8, 32)


def other(axis):
    return {axis: 1 - lax.axis_index(axis)}


def offset_peer(dd):
    peer = {}
    for bit, axis in ((4, 'slab'), (2, 'col'), (1, 'row')):
        here = lax.axis_index(axis)
        peer[axis] = 1 - here if dd & bit else here
    return peer


def tree(parts):
    while len(parts) > 1:
        parts = [parts[k] + parts[k + 1] for k in range(0, len(parts), 2)]
    return parts[0]


def kernel(snaps, rows, x_hbm, f1_hbm, f2_hbm, f3_hbm, g_out, e_out,
           xbuf, f1, f2, f3, u3w, u2w, w1, own, ysend, yrecv, bown, xsend, xrecv,
           gpart, grecv, ex, energy, glast, u2n, w1o, blast, x_sem, ys_sem, yr_sem, xs_sem, xr_sem, g_sem, all_send, all_recv, ylr_sem):
    nq = 128 // rows
    nc = snaps * nq
    width = rows * 8
    last = snaps - 1
    slab, col, row = (lax.axis_index(a) for a in ('slab', 'col', 'row'))

    def x_copy(c):
        slot = lax.rem(c, XBUF)
        return pltpu.make_async_copy(x_hbm.at[c], xbuf.at[slot], x_sem.at[slot])

    f_copies = [pltpu.make_async_copy(src, dst, all_send.at[k]) for k, (src, dst) in enumerate(((f3_hbm, f3), (f2_hbm, f2), (f1_hbm, f1)))]
    pieces = rows // SUB
    spans = list(zip(FIRST[:-1], FIRST[1:]))
    x_first = []
    for k, (begin, end) in enumerate(spans):
        part = pl.ds(begin * 128, (end - begin) * 128)
        x_first.append(pltpu.make_async_copy(x_hbm.at[0, part], xbuf.at[0, part], x_sem.at[k] if k < XBUF else xs_sem.at[k - XBUF]))
    x_first[0].start()
    f_copies[0].start()
    for copy in x_first[1:]:
        copy.start()

    barrier = pltpu.get_barrier_semaphore()
    for dd in (4, 2, 1):
        pl.semaphore_signal(barrier, inc=1, device_id=offset_peer(dd), device_id_type=MESH)

    def swapped(block, flip):
        return jnp.where(flip == 0, block, jnp.concatenate([block[8:], block[:8]], axis=0)).astype(BF16)

    f_copies[0].wait()
    u3w[...] = swapped(f3[:, pl.ds(pl.multiple_of(slab * 128, 128), 128)], slab)
    ex[...] = jnp.zeros_like(ex)

    def y_copy(c):
        held, slot = lax.rem(c, HELD), lax.rem(c, RING)
        return pltpu.make_async_remote_copy(ysend.at[held], yrecv.at[slot], ys_sem.at[lax.rem(c, LAG)], yr_sem.at[slot], device_id=other('slab'), device_id_type=MESH)

    def b_copy(c):
        held, slot = lax.rem(c, BHELD), lax.rem(c, BRING)
        return pltpu.make_async_remote_copy(xsend.at[held], xrecv.at[slot], xs_sem.at[held], xr_sem.at[slot], device_id=other('col'), device_id_type=MESH)

    def y_first(k):
        begin, end = spans[k]
        part = pl.ds(begin, end - begin)
        return pltpu.make_async_remote_copy(ysend.at[0, part], yrecv.at[0, part], ys_sem.at[0], yr_sem.at[0], device_id=other('slab'), device_id_type=MESH)

    def y_last(k):
        part = pl.ds(k * (rows // LAST), rows // LAST)
        return pltpu.make_async_remote_copy(ysend.at[(nc - 1) % HELD, part], yrecv.at[(nc - 1) % RING, part], ys_sem.at[(nc - 1) % LAG], yr_sem.at[(nc - 1) % RING] if k == 0 else ylr_sem.at[k - 1], device_id=other('slab'), device_id_type=MESH)

    def to_each(send):
        for dest in range(8):
            place = {'slab': dest // 4, 'col': dest // 2 % 2, 'row': dest % 2}
            bits = [lax.axis_index(a) if there == 0 else 1 - lax.axis_index(a) for a, there in place.items()]
            slot = bits[0] * 4 + bits[1] * 2 + bits[2]

            @pl.when(slot > 0)
            def _():
                send(slot, bits[0], place).start()

    def wide_copy(k):
        return lambda slot, far, place: pltpu.make_async_remote_copy(blast.at[0, k], blast.at[slot, k], all_send.at[0], all_recv.at[far], device_id=place, device_id_type=MESH)

    def energy_copy(slot, far, place):
        return pltpu.make_async_remote_copy(energy.at[0], energy.at[slot], all_send.at[2], all_recv.at[4], device_id=place, device_id_type=MESH)

    def last_copy(slot, far, place):
        return pltpu.make_async_remote_copy(gpart.at[last], glast.at[slot], all_send.at[1], all_recv.at[2 + far], device_id=place, device_id_type=MESH)

    def wait_all(buffer, begin, end, sem):
        part = buffer.at[pl.ds(begin, end - begin)]
        pltpu.make_async_copy(part, part, sem).wait()

    early = pl.ds(0, last)
    g_copy = pltpu.make_async_remote_copy(gpart.at[early], grecv.at[early], all_send.at[2], g_sem.at[0], device_id=other('row'), device_id_type=MESH)

    def block(slot, xs, begin, count):
        x = xbuf[xs, pl.ds(begin * 128, count * 128), :]
        part = lax.dot_general(u3w[...], x, NT, preferred_element_type=F32)
        for i in range(count):
            own[slot, begin + i] = part[:8, i * 128:(i + 1) * 128]
            ysend[slot, begin + i] = part[8:, i * 128:(i + 1) * 128]
        xf = x.astype(F32).reshape(-1, 4, 8, 128)
        return jnp.sum(xf * xf, axis=0)

    def mode_three(c):
        slot, xs = lax.rem(c, HELD), lax.rem(c, XBUF)
        x_copy(c).wait()
        acc = lax.fori_loop(0, pieces, lambda k, acc: acc + block(slot, xs, pl.multiple_of(k * SUB, SUB), SUB), jnp.zeros((4, 8, 128), F32))
        t = lax.div(c, nq)
        ex[t] += jnp.sum(acc, axis=0)

        @pl.when(c + XBUF < nc)
        def _():
            x_copy(c + XBUF).start()

    def mode_two(c):
        bslot = lax.rem(c, BHELD)

        @pl.when(c >= BHELD)
        def _():
            b_copy(c).wait_send()

        y_copy(c).wait_recv()
        a = (own[lax.rem(c, HELD)] + yrecv[lax.rem(c, RING)]).reshape(width, 128).astype(BF16)
        part = lax.dot_general(u2w[...], a, NT, preferred_element_type=F32)
        bown[bslot] = part[:8]
        xsend[bslot] = part[8:]
        b_copy(c).start()

    def mode_one(c):
        b_copy(c).wait_recv()
        b = (bown[lax.rem(c, BHELD)] + xrecv[lax.rem(c, BRING)]).astype(BF16)
        q, t = lax.rem(c, nq), lax.div(c, nq)
        g = jnp.dot(b, w1[q], preferred_element_type=F32)

        @pl.when(q == 0)
        def _():
            gpart[t] = g

        @pl.when(q > 0)
        def _():
            gpart[t] += g

    def late_setup():
        f_copies[1].wait()
        f_copies[2].wait()
        block_two = f2[:, pl.ds(pl.multiple_of(col * 128, 128), 128)]
        u2n[...] = block_two.astype(BF16)
        u2w[...] = swapped(block_two, col)
        spread = (lax.broadcasted_iota(jnp.int32, (16, 128), 1) // 8 == lax.broadcasted_iota(jnp.int32, (16, 128), 0)).astype(BF16)
        r = lax.broadcasted_iota(jnp.int32, (width, 128), 0)
        l = lax.broadcasted_iota(jnp.int32, (width, 128), 1)

        def diagonal(which, q):
            u1 = f1[:, pl.ds(pl.multiple_of(which * 128, 128), 128)].astype(BF16)
            pick = (l == q * rows + r // 8).astype(BF16)
            rowed = lax.dot_general(pick, u1, NT, preferred_element_type=F32).astype(BF16)
            wide = jnp.dot(rowed, spread, preferred_element_type=F32)
            return jnp.where(r % 8 == l % 8, wide, 0.0).astype(BF16)

        for q in range(nq):
            w1[q] = diagonal(row, q)
        w1o[...] = diagonal(1 - row, nq - 1)

    def as_row(column, count):
        i = lax.broadcasted_iota(jnp.int32, (count, 128), 0)
        return jnp.sum(jnp.where(i == lax.broadcasted_iota(jnp.int32, (count, 128), 1), column, 0.0), axis=0, keepdims=True)

    def row_sums(blocks):
        return as_row(jnp.sum(jnp.sum(blocks, axis=1), axis=1, keepdims=True), blocks.shape[0])

    def step(s, carry):
        @pl.when((s > LAG) & (s <= nc))
        def _():
            y_copy(s - 1 - LAG).wait_send()

        @pl.when((s >= 2) & (s < nc))
        def _():
            y_copy(s - 1).start()

        @pl.when(s == nc)
        def _():
            for k in range(LAST):
                y_last(k).start()

        @pl.when(s < nc)
        def _():
            mode_three(s)

        @pl.when(s == 2)
        def _():
            late_setup()

        @pl.when(s == nc)
        def _():
            energy[0, :1] = row_sums(ex[...])

        @pl.when(s == nc + LAG - 3)
        def _():
            g_copy.start()

        @pl.when(s >= LAG)
        def _():
            mode_two(s - LAG)

        @pl.when(s == nc + LAG - 2)
        def _():
            g_copy.wait()
            g = gpart[early] + grecv[early]
            grecv[early] = g
            energy[0, 1:] = row_sums(g * g)

        @pl.when(s >= LAG + 1)
        def _():
            mode_one(s - LAG - 1)

        return carry

    first = jnp.zeros((4, 8, 128), F32)
    for k, (begin, end) in enumerate(spans):
        x_first[k].wait()
        if k == 0:
            f_copies[1].start()
            f_copies[2].start()
        elif k < XBUF:
            x_copy(k).start()
        first += block(0, 0, begin, end - begin)
        if k == 0:
            pl.semaphore_wait(barrier, 3)
        y_first(k).start()
    ex[0] = jnp.sum(first, axis=0)
    x_copy(XBUF).start()
    lax.fori_loop(1, nc + LAG - 1, step, 0)

    to_each(energy_copy)
    for k in range(LAST):
        if k == LAST - 1:
            mode_one(nc - 2)
            to_each(last_copy)
        y_last(k).wait_recv()
        part = pl.ds(k * (rows // LAST), rows // LAST)
        a = (own[(nc - 1) % HELD, part] + yrecv[(nc - 1) % RING, part]).reshape(width // LAST, 128).astype(BF16)
        blast[0, k] = lax.dot_general(u2n[...], a, NT, preferred_element_type=F32)
        to_each(wide_copy(k))

    def chip_pair(base):
        def summed(first):
            return jnp.concatenate([blast[first, k] + blast[first + 2, k] for k in range(LAST)], axis=1).astype(BF16)

        b_here, b_twin = summed(base), summed(base + 1)
        part = jnp.dot(b_here, w1[nq - 1], preferred_element_type=F32) + jnp.dot(b_twin, w1o[...], preferred_element_type=F32)
        low, high = part[:8], part[8:]
        return jnp.where(col == 0, low, high), jnp.where(col == 0, high, low)

    wait_all(glast, 1, 4, all_recv.at[2])
    wait_all(blast, 1, 4, all_recv.at[0])
    near = chip_pair(0)
    mine = (gpart[last] + glast[1]) + near[0]
    grecv[last] = mine
    for b in range(8):
        turned = grecv[:, b, :].T
        g_out[:, b] = jnp.where(row == 0, turned[:64], turned[64:]).reshape(8, 8, snaps)
    wait_all(energy, 1, 8, all_recv.at[4])
    x_energy = tree([energy[dd, :1] for dd in range(8)])
    g_energy = tree([energy[dd, 1:] for dd in (0, 2, 4, 6)])
    wait_all(glast, 4, 8, all_recv.at[3])
    wait_all(blast, 4, 8, all_recv.at[1])
    far = chip_pair(4)
    chips = [mine] + [(glast[dd] + glast[dd + 1]) + add for dd, add in ((2, near[1]), (4, far[0]), (6, far[1]))]
    final = jnp.sum(jnp.sum(tree([g * g for g in chips]), axis=0, keepdims=True), axis=1, keepdims=True)
    g_energy = jnp.where(lax.broadcasted_iota(jnp.int32, (1, 128), 1) == last, final, g_energy)
    e_out[...] = ((x_energy - g_energy) / x_energy)[:, :snaps]

    for c in range(nc - LAG, nc):
        y_copy(c).wait_send()
    for c in range(nc - 1 - BHELD, nc - 1):
        b_copy(c).wait_send()
    wait_all(energy, 1, 8, all_send.at[2])
    wait_all(glast, 1, 8, all_send.at[1])
    wait_all(blast, 1, 8, all_send.at[0])


def finish(g_in, e_in, g_out, e_out, sem):
    copies = [pltpu.make_async_copy(g_in, g_out, sem.at[0]), pltpu.make_async_copy(e_in, e_out, sem.at[1])]
    for copy in copies:
        copy.start()
    for copy in copies:
        copy.wait()


def solution(mesh):
    rows = 32

    def local_part(x_block, f_one, f_two, f_three):
        snaps = x_block.shape[0]
        nq = 128 // rows
        nc = snaps * nq
        dma = pltpu.SemaphoreType.DMA
        hbm = pl.BlockSpec(memory_space=pltpu.HBM)
        vmem = pl.BlockSpec(memory_space=pltpu.VMEM)
        g, e = pl.pallas_call(
            functools.partial(kernel, snaps, rows),
            out_shape=(pltpu.VMEM((8, 8, 8, snaps), F32), pltpu.VMEM((1, snaps), F32)),
            in_specs=[hbm] * 4,
            out_specs=(vmem, vmem),
            scratch_shapes=[
                pltpu.VMEM((XBUF, rows * 128, 128), BF16),
                pltpu.VMEM((16, 256), F32), pltpu.VMEM((16, 256), F32), pltpu.VMEM((16, 256), F32),
                pltpu.VMEM((16, 128), BF16), pltpu.VMEM((16, 128), BF16),
                pltpu.VMEM((nq, rows * 8, 128), BF16),
                pltpu.VMEM((HELD, rows, 8, 128), F32), pltpu.VMEM((HELD, rows, 8, 128), F32), pltpu.VMEM((RING, rows, 8, 128), F32),
                pltpu.VMEM((BHELD, 8, rows * 8), F32), pltpu.VMEM((BHELD, 8, rows * 8), F32), pltpu.VMEM((BRING, 8, rows * 8), F32),
                pltpu.VMEM((snaps, 8, 128), F32), pltpu.VMEM((snaps, 8, 128), F32),
                pltpu.VMEM((snaps, 8, 128), F32), pltpu.VMEM((8, 2, 128), F32), pltpu.VMEM((8, 8, 128), F32),
                pltpu.VMEM((16, 128), BF16), pltpu.VMEM((rows * 8, 128), BF16), pltpu.VMEM((8, LAST, 16, rows * 8 // LAST), F32),
                dma((XBUF,)), dma((LAG,)), dma((RING,)), dma((BHELD,)), dma((BRING,)), dma((1,)), dma((3,)), dma((5,)), dma((LAST - 1,)),
            ],
            compiler_params=pltpu.CompilerParams(collective_id=0, has_side_effects=True, vmem_limit_bytes=40 * 1024 * 1024),
        )(x_block.reshape(nc, rows * 128, 128), *(pltpu.with_memory_space_constraint(f.T, pltpu.HBM) for f in (f_one, f_two, f_three)))
        g, e = pl.pallas_call(
            finish,
            out_shape=(jax.ShapeDtypeStruct((8, 8, 8, snaps), F32), jax.ShapeDtypeStruct((1, snaps), F32)),
            in_specs=[vmem] * 2,
            out_specs=(hbm, hbm),
            scratch_shapes=[dma((2,))],
            compiler_params=pltpu.CompilerParams(vmem_limit_bytes=4 * 1024 * 1024),
        )(*(pltpu.with_memory_space_constraint(r, pltpu.VMEM) for r in (g, e)))
        return g.transpose(3, 0, 1, 2), e.reshape(snaps)

    return jax.shard_map(local_part, mesh=mesh, in_specs=(P(None, 'row', 'col', 'slab'), P(None, None), P(None, None), P(None, None)), out_specs=(P(None, 'row', 'col', 'slab'), P()), check_vma=False)
```
